512 devices in a mesh: lat: 64 (over y, z), ma: 8 (over x, core).
Axes of the slice: x: 4, y: 8, z: 8, core: 2. Of those that a mesh axis runs over, the one named last changes fastest.
Arguments:
- pair_wave: int32 [360], replicated, may hold values from 0 to 359, each once
- legendre: bfloat16 [360, 640, 768], P('ma', 'lat'), may hold values from -0.0078125 to 0.0078125
- coefs: bfloat16 [360, 768, 168], P('ma', 'lat'), may hold values from -6 to 6
Outputs:
- noise: float32 [53760, 1440], P(('lat', 'ma'))
The draws below stay inside these ranges and needn't reach their ends.
Inputs may be any that keep to these rules, and one draw needn't show every extreme that they name: Slot q holds wavenumbers pair_wave[q] and 719 - pair_wave[q]; every value appears once.
All inputs are finite; a program needn't handle non-finite values.
Results may differ from the reference program's by a relative error of at most 0.0003.
Values may be sent and summed in bfloat16 or wider, within the bound.
A program may use at most 64 MiB of HBM per device.

```python
import math
import jax
import jax.numpy as jnp
from jax import lax

DEG = 720
LON = 1440
CH = 84
LAT_DEV = 10
PAIRS = 360
RROWS = 768
COLS = 168
LATS = 640
N_LAT = 64
N_MA = 8


def level_of(key, dims, split, smallest, high):
    factor_of = 1.0
    for axis_at, shards_of in split:
        draws = jax.random.uniform(jax.random.fold_in(jax.random.fold_in(key, 6), axis_at), (shards_of,), jnp.float32, smallest / len(split), high / len(split))
        factor_of = factor_of * jnp.repeat(jnp.exp(draws), dims[axis_at] // shards_of).reshape((-1,) + (1,) * (len(dims) - 1 - axis_at))
    return factor_of


def noise(stream_key, extent, deviation, most, shards=(), kind=jnp.bfloat16):
    values = jax.random.normal(stream_key, extent, jnp.float32) * deviation
    if len(shards) > 0:
        values = level_of(stream_key, extent, shards, -0.22, 0.18) * values
    return jnp.clip(values, min=-most, max=most).astype(kind)


def setup_inputs(seed: int = 0) -> dict:
    key_list = jax.random.split(jax.random.key(seed), 4)
    pair_wave = jax.random.permutation(key_list[0], PAIRS).astype(jnp.int32)
    legendre = noise(key_list[1], (PAIRS, LATS, RROWS), (RROWS * DEG) ** -0.5, 0.0078125, ((0, 8), (1, 64)))
    coefs = noise(key_list[2], (PAIRS, RROWS, COLS), 1.0, 6.0, ((0, 8), (1, 64)))
    return dict(pair_wave=pair_wave, legendre=legendre, coefs=coefs)


def chain_table(table, wave_ids, degree_top):
    row_count = table.shape[2]
    row_ids = jnp.arange(row_count, dtype=jnp.int32)[None, :]
    split_row = (degree_top - wave_ids).astype(jnp.int32)[:, None]
    inside = row_ids < split_row
    outside = (row_ids >= split_row) & (row_ids <= degree_top)
    masks = jnp.stack([inside, outside], axis=1)
    return jnp.where(masks[:, :, None, :], table[:, None, :, :], jnp.zeros((), table.dtype))


def fourier_basis(pair_wave, degree_top, lon_count):
    orders = jnp.stack([pair_wave, degree_top - 1 - pair_wave], axis=1).astype(jnp.int32)
    positions = jnp.arange(lon_count, dtype=jnp.int32)
    phase_int = (orders[:, :, None] * positions[None, None, :]) % lon_count
    radians = (2.0 * math.pi / lon_count) * phase_int.astype(jnp.float32)
    weight = jnp.where(orders == 0, 1.0, 2.0).astype(jnp.float32)[:, :, None]
    real_row = weight * jnp.cos(radians)
    imag_row = -weight * jnp.sin(radians)
    return jnp.stack([real_row, imag_row], axis=2).reshape(-1, lon_count)


def reference(pair_wave, legendre, coefs):
    pair_count = pair_wave.shape[0]
    row_count = coefs.shape[1]
    lat_total = LAT_DEV * N_LAT
    slot_count = pair_count // N_MA

    def group_spectra(packed):
        wave_ids, group_table, group_coefs = packed
        masked = chain_table(group_table, wave_ids, DEG)
        return jnp.einsum('qeir,qrc->qeic', masked.astype(jnp.float32), group_coefs.astype(jnp.float32), precision=lax.Precision.HIGHEST)

    spectra = lax.map(group_spectra, (pair_wave.reshape(N_MA, slot_count), legendre.reshape(N_MA, slot_count, lat_total, row_count), coefs.reshape(N_MA, slot_count, row_count, coefs.shape[2])))
    spectra = spectra.reshape(pair_count, 2, lat_total, 2, CH)
    fourier_rows = jnp.transpose(spectra, (0, 1, 3, 2, 4)).reshape(4 * pair_count, lat_total * CH)
    synth_basis = fourier_basis(pair_wave, DEG, LON)
    return lax.dot_general(fourier_rows, synth_basis, (((0,), (0,)), ((), ())), precision=lax.Precision.HIGHEST)
```

```python
import functools
import math

import jax
import jax.numpy as jnp
from jax import lax
from jax.experimental import pallas as pl
from jax.experimental.pallas import tpu as pltpu
from jax.sharding import PartitionSpec as P

LON = 1440
HALF = 720
RING = 8
ORDER = (1, 7, 2, 6, 3, 5, 4)
GROUP = 6
CH = 84
SINE = [(-1.0) ** n / math.factorial(2 * n + 1) for n in range(6)]
MESH = pl.DeviceIdType.MESH


def split_bf16(x):
    hi = lax.reduce_precision(x, 8, 7)
    return hi.astype(jnp.bfloat16), (x - hi).astype(jnp.bfloat16)


def basis_rows(waves, quarter):
    positions = jnp.arange(HALF, dtype=jnp.int32).astype(jnp.float32)
    order = waves.astype(jnp.float32)
    phase = order[:, None] * positions[None, :] + quarter.astype(jnp.float32)[:, None]
    turns = jnp.round(phase * (1.0 / LON))
    angle = (phase - turns * LON) * (math.pi / LON)
    square = angle * angle
    poly = jnp.float32(SINE[-1])
    for coefficient in SINE[-2::-1]:
        poly = poly * square + coefficient
    sine = angle * poly
    weight = jnp.where(waves == 0, 1.0, 2.0).astype(jnp.float32)[:, None]
    return split_bf16(weight - (2.0 * weight) * (sine * sine))


def pack_table(legendre):
    slots, rows_dev, row_count = legendre.shape
    table = jnp.pad(legendre, ((0, RING * GROUP - slots), (0, 0), (0, 0)))
    head = table[:, :8].reshape(RING, 2, 24, row_count)
    tail = table[:, 8:].reshape(RING, 2, 6, row_count)
    tail = jnp.pad(tail, ((0, 0), (0, 0), (0, 2), (0, 0)))
    return jnp.concatenate([head, tail], axis=2)


def pack_coefs(coefs):
    slots, deg_dev, cols = coefs.shape
    x = jnp.pad(coefs, ((0, RING * GROUP - slots), (0, 0), (0, 0)))
    x = x.reshape(RING, 2, 3, deg_dev, 2, CH).transpose(0, 1, 4, 3, 2, 5)
    x = x.reshape(RING, 2, 2, deg_dev, 3 * CH)
    x = jnp.pad(x, ((0, 0),) * 4 + ((0, 256 - 3 * CH),))
    x = x.reshape(RING, 2, 2, deg_dev, 2, 128).transpose(0, 1, 2, 4, 3, 5)
    return x.reshape(RING, 8 * deg_dev, 128)


def sums_kernel(
    waves, table, packs, out,
    table_in, packs_in, wide, coef_rows, coef_all, coded, back,
    c_send, c_recv, l_send, l_recv, r_send, r_recv,
    b_send, b_recv, m_send, m_recv, local,
):
    lat = lax.axis_index("lat")
    ma = lax.axis_index("ma")
    y = lat // RING
    z = lax.rem(lat, RING)
    z_to = [lax.rem(z + d, RING) for d in ORDER]
    z_from = [lax.rem(z + RING - d, RING) for d in ORDER]
    ma_to = [lax.rem(ma + d, RING) for d in ORDER]
    up = (lax.rem(y + 1, RING) * RING + z, ma)
    down = (lax.rem(y + RING - 1, RING) * RING + z, ma)

    barrier = pltpu.get_barrier_semaphore()
    targets = [(y * RING + p, ma) for p in z_to] + [(lat, p) for p in ma_to] + [up, down]
    for target in targets:
        pl.semaphore_signal(barrier, inc=1, device_id=target, device_id_type=MESH)
    pl.semaphore_wait(barrier, len(targets))

    def remote(src, dst, send, recv, target):
        copy = pltpu.make_async_remote_copy(
            src_ref=src, dst_ref=dst, send_sem=send, recv_sem=recv,
            device_id=target, device_id_type=MESH,
        )
        copy.start()
        return copy

    c_copies = [
        remote(packs.at[p], packs_in.at[z], c_send.at[k], c_recv.at[k], (y * RING + p, ma))
        for k, p in enumerate(z_to)
    ]
    own_c = pltpu.make_async_copy(packs.at[z], packs_in.at[z], local.at[0])
    own_c.start()
    own_l = pltpu.make_async_copy(table.at[z], table_in.at[z], local.at[1])
    own_l.start()
    l_copies = []
    for a in range(2):
        for k, p in enumerate(z_to):
            l_copies.append(
                remote(table.at[p, a], table_in.at[z, a], l_send.at[a, k], l_recv.at[a, k], (y * RING + p, ma))
            )

    own_c.wait()
    for copy in c_copies:
        copy.wait_recv()
    deg_dev = packs.shape[1] // 8
    for s in range(RING):
        wide[s] = packs_in[s].astype(jnp.float32)
    for a in range(2):
        for s in range(RING):
            for t in range(4):
                piece = wide[s, pl.ds((a * 4 + t) * deg_dev, deg_dev), :]
                coef_rows[a, pl.ds(s * deg_dev, deg_dev), pl.ds(t * 128, 128)] = piece
        coef_all[y, a] = coef_rows[a].astype(jnp.bfloat16)

    piece_rows = coef_all.shape[2] // 2

    def ring_send(dirn, step, s):
        org = lax.rem(y + (RING - step if dirn == 0 else step), RING)
        ref = coef_all.at[org, s // 2, pl.ds((s % 2) * piece_rows, piece_rows)]
        return remote(ref, ref, r_send.at[dirn, step, s], r_recv.at[dirn, step, s], up if dirn == 0 else down)

    def hops(dirn, s):
        return 4 if (s % 2 == 0) == (dirn == 0) else 3

    live = {}
    for s in range(4):
        for dirn in range(2):
            live[dirn, 0, s] = ring_send(dirn, 0, s)
    for step in range(1, 5):
        for s in range(4):
            for dirn in range(2):
                if step <= hops(dirn, s):
                    live[dirn, step - 1, s].wait_recv()
                    if step < hops(dirn, s):
                        live[dirn, step, s] = ring_send(dirn, step, s)

    own_l.wait()
    for copy in l_copies:
        copy.wait_recv()

    row = lax.broadcasted_iota(jnp.int32, (32, 1), 0)
    member = jnp.where(row < 24, row // 8, (row - 24) // 2)
    column = lax.broadcasted_iota(jnp.int32, (1, 1, table.shape[3]), 2)
    lane = lax.rem(lax.broadcasted_iota(jnp.int32, (1, 1, 512), 2), 256)
    lane_out = lax.broadcasted_iota(jnp.int32, (1, 1, 128), 2)
    last = waves.shape[0] // RING - 1
    for a in range(2):
        bounds = []
        for b in range(3):
            slot = jnp.minimum(z * GROUP + a * 3 + b, last)
            u = waves[ma * (last + 1) + slot]
            cut = HALF - u
            even = (u & 1) == 0
            bounds.append((
                (jnp.where(even, 0, cut), jnp.where(even, cut, HALF + 1)),
                (jnp.where(even, cut, 0), jnp.where(even, HALF + 1, cut)),
            ))
        rows_a = table_in[:, a].astype(jnp.float32)
        rhs = coef_all[:, a].reshape(-1, 512)
        for par in range(2):
            low, high = [
                jnp.where(member == 0, bounds[0][par][j], jnp.where(member == 1, bounds[1][par][j], bounds[2][par][j]))[None]
                for j in range(2)
            ]
            keep = (column >= low) & (column < high)
            lhs = jnp.where(keep, rows_a, 0.0).astype(jnp.bfloat16).reshape(256, -1)
            sums = jnp.dot(lhs, rhs, preferred_element_type=jnp.float32)
            sums = sums.reshape(RING, 4, 8, 512)
            tail = sums[:, 3]
            two, four = pltpu.roll(tail, 6, 1), pltpu.roll(tail, 4, 1)
            parts = (
                (0, 8, (sums[:, 0], sums[:, 1], sums[:, 2])),
                (8, 2, (tail, two, four)),
            )
            for start, count, (s0, s1, s2) in parts:
                value = jnp.where(lane < CH, s0, jnp.where(lane < 2 * CH, s1, s2))
                value = jnp.where(lane < 3 * CH, value, 0.0)
                top = jnp.max(jnp.abs(value), axis=2, keepdims=True)
                power = jnp.ceil(jnp.log2(jnp.maximum(top, 1e-30)) + 1e-3)
                code = jnp.round(value * (jnp.exp2(-power) * 32767.0)).astype(jnp.int32)
                word = (code[:, :, :256] << 16) | (code[:, :, 256:] & 0xFFFF)
                first, second = word[:, :, :128], word[:, :, 128:]
                second = jnp.where(lane_out == 3 * CH - 128, power.astype(jnp.int32), second)
                for half, item in enumerate((first, second)):
                    coded[:, start : start + count, a * 4 + par * 2 + half, :] = item[:, :count]

    b_copies = [
        remote(coded.at[p], back.at[z], b_send.at[k], b_recv.at[k], (y * RING + p, ma))
        for k, p in enumerate(z_to)
    ]
    m_copies = []
    own = []

    def forward(k, src, zs):
        for j, p in enumerate(ma_to):
            m_copies.append(
                remote(src.at[pl.ds((5 * p) // 4, 2)], out.at[ma, zs], m_send.at[k, j], m_recv.at[k, j], (lat, p))
            )
        copy = pltpu.make_async_copy(src.at[pl.ds((5 * ma) // 4, 2)], out.at[ma, zs], local.at[2 + k])
        copy.start()
        own.append(copy)

    forward(7, coded.at[z], z)
    for k, zs in enumerate(z_from):
        b_copies[k].wait_recv()
        forward(k, back.at[zs], zs)
    for copy in c_copies + l_copies + list(live.values()) + b_copies:
        copy.wait_send()
    for copy in own:
        copy.wait()
    for copy in m_copies:
        copy.wait()


def sums_call(waves, table, packs):
    vmem = pl.BlockSpec(memory_space=pltpu.VMEM)
    dma = pltpu.SemaphoreType.DMA
    deg = packs.shape[1] // 8 * RING
    return pl.pallas_call(
        sums_kernel,
        out_shape=jax.ShapeDtypeStruct((RING, RING, 2, 8, 128), jnp.int32),
        in_specs=[pl.BlockSpec(memory_space=pltpu.SMEM), vmem, vmem],
        out_specs=vmem,
        scratch_shapes=[
            pltpu.VMEM(table.shape, jnp.bfloat16),
            pltpu.VMEM(packs.shape, jnp.bfloat16),
            pltpu.VMEM(packs.shape, jnp.float32),
            pltpu.VMEM((2, deg, 512), jnp.float32),
            pltpu.VMEM((RING, 2, deg, 512), jnp.bfloat16),
            pltpu.VMEM((RING, 10, 8, 128), jnp.int32),
            pltpu.VMEM((RING, 10, 8, 128), jnp.int32),
            dma((7,)), dma((7,)), dma((2, 7)), dma((2, 7)),
            dma((2, 4, 4)), dma((2, 4, 4)),
            dma((7,)), dma((7,)), dma((8, 7)), dma((8, 7)), dma((10,)),
        ],
        compiler_params=pltpu.CompilerParams(
            collective_id=0, has_side_effects=True, vmem_limit_bytes=40 << 20
        ),
        name="sums",
    )(waves, table, packs)


def body(pair_wave, legendre, coefs):
    ma_i = lax.axis_index("ma")
    slots = legendre.shape[0]
    table, packs = pack_table(legendre), pack_coefs(coefs)
    local = jnp.minimum(jnp.arange(RING * GROUP), slots - 1)
    waves = pair_wave.reshape(RING, slots)[:, local]
    even = jnp.where(waves % 2 == 0, waves, HALF - 1 - waves).reshape(-1)
    orders = jnp.stack([even, even, HALF - 1 - even, HALF - 1 - even])
    quarters = jnp.broadcast_to(jnp.array([[0], [LON // 4]] * 2), orders.shape)
    hi, lo = basis_rows(orders.reshape(-1), quarters.reshape(-1))
    hi, lo = hi.reshape(2, -1, HALF), lo.reshape(2, -1, HALF)
    basis = jnp.concatenate([hi, lo, hi], axis=1)

    words = sums_call(pair_wave, table, packs)
    words = words.reshape(RING, RING, 2, 2, 2, 256)
    power = words[..., 3 * CH : 3 * CH + 1]
    scale = jnp.exp2(power.astype(jnp.float32)) * (1.0 / 32767.0)
    words = words[..., : 3 * CH]
    both = jnp.stack([words >> 16, (words << 16) >> 16])
    value = both.astype(jnp.float32) * scale[None]
    value = value.reshape(2, RING, RING, 2, 2, 2, 3, CH)
    value = value.transpose(5, 0, 1, 2, 4, 6, 3, 7).reshape(2, -1, 2 * CH)
    hi, lo = split_bf16(value)
    rows = jnp.concatenate([hi, hi, lo], axis=1)
    both = lax.dot_general(
        rows, basis, (((1,), (1,)), ((0,), (0,))), preferred_element_type=jnp.float32
    )
    start = 105 * ma_i - CH * ((5 * ma_i) // 4)
    both = lax.dynamic_slice_in_dim(both, start, 105, axis=1)
    return jnp.concatenate([both[0] + both[1], both[0] - both[1]], axis=1)


def solution(mesh):
    in_specs = (P(), P("ma", "lat", None), P("ma", "lat", None))
    out_specs = P(("lat", "ma"), None)
    return jax.shard_map(body, mesh=mesh, in_specs=in_specs, out_specs=out_specs, check_vma=False)
```

```python
import math

import jax
import jax.numpy as jnp
from jax import lax
from jax.experimental import pallas as pl
from jax.experimental.pallas import tpu as pltpu
from jax.sharding import PartitionSpec as P

LON = 1440
HALF = 720
RING = 8
ORDER = (1, 7, 2, 6, 3, 5, 4)
TABLE_STEPS = ((4, 5), (2, 3), (6,), (0, 1))
BASIS_STEPS = (3, 2, 1, 0)
CH = 84
SINE = [(-1.0) ** n / math.factorial(2 * n + 1) for n in range(6)]
COSINE = [(-1.0) ** n / math.factorial(2 * n) for n in range(7)]
MESH = pl.DeviceIdType.MESH


def pack_table(legendre):
    slots, rows_dev, row_count = legendre.shape
    table = jnp.pad(legendre, ((0, 6 * RING - slots), (0, 0), (0, 0)))
    head = table[:, :8].reshape(2, RING, 24, row_count)
    tail = table[:, 8:].reshape(2, RING, 6, row_count)
    tail = jnp.pad(tail, ((0, 0), (0, 0), (0, 2), (0, 0)))
    return jnp.concatenate([head, tail], axis=2)


def pack_coefs(coefs):
    slots, deg_dev, cols = coefs.shape
    x = jnp.pad(coefs, ((0, 6 * RING - slots), (0, 0), (0, 0)))
    x = x.reshape(2, RING, 3, deg_dev, 2, CH).transpose(0, 1, 4, 3, 2, 5)
    x = x.reshape(2, RING, 2, deg_dev, 3 * CH)
    x = jnp.pad(x, ((0, 0),) * 4 + ((0, 256 - 3 * CH),))
    x = x.reshape(2, RING, 2, deg_dev, 2, 128).transpose(0, 1, 2, 4, 3, 5)
    return x.reshape(2, RING, 4 * deg_dev, 128)


def poly(coefficients, square):
    value = jnp.float32(coefficients[-1])
    for coefficient in coefficients[-2::-1]:
        value = value * square + coefficient
    return value


def turn(phase):
    turns = jnp.round(phase * (1.0 / LON))
    angle = (phase - turns * LON) * (math.pi / LON)
    square = angle * angle
    sine = angle * poly(SINE, square)
    return 1.0 - 2.0 * (sine * sine), 2.0 * (sine * poly(COSINE, square))


def split_bf16(x):
    hi = x.astype(jnp.bfloat16)
    return hi, (x - hi.astype(jnp.float32)).astype(jnp.bfloat16)


def synth_kernel(
    waves, table, packs, out,
    table_in, packs_in, wide, coef_rows, coef_all, coded, back, words,
    perm, orders, basis, turned, rows, total,
    c_send, c_recv, l_send, l_recv, r_send, r_recv,
    b_send, b_recv, m_send, m_recv, local,
):
    lat = lax.axis_index("lat")
    ma = lax.axis_index("ma")
    y = lat // RING
    z = lax.rem(lat, RING)
    group = (z, y)
    place = (y, z)
    to = [[lax.rem(group[a] + d, RING) for d in ORDER] for a in range(2)]
    source = [[lax.rem(group[a] + RING - d, RING) for d in ORDER] for a in range(2)]
    ma_to = [lax.rem(ma + d, RING) for d in ORDER]

    def peer(a, p):
        return (y * RING + p, ma) if a == 0 else (p * RING + z, ma)

    next_to = [
        [peer(1 - a, lax.rem(place[a] + step, RING)) for step in (1, RING - 1)]
        for a in range(2)
    ]

    barrier = pltpu.get_barrier_semaphore()
    targets = [peer(a, p) for a in range(2) for p in to[a]] + [(lat, p) for p in ma_to]
    for target in targets:
        pl.semaphore_signal(barrier, inc=1, device_id=target, device_id_type=MESH)
    pl.semaphore_wait(barrier, len(targets))

    def remote(src, dst, send, recv, target):
        copy = pltpu.make_async_remote_copy(
            src_ref=src, dst_ref=dst, send_sem=send, recv_sem=recv,
            device_id=target, device_id_type=MESH,
        )
        copy.start()
        return copy

    def keep_local(src, dst, sem):
        copy = pltpu.make_async_copy(src, dst, sem)
        copy.start()
        return copy

    c_copies = [[], []]
    for k in range(7):
        for a in range(2):
            p = to[a][k]
            c_copies[a].append(
                remote(packs.at[a, p], packs_in.at[a, group[a]], c_send.at[a, k], c_recv.at[a, k], peer(a, p))
            )
    own_c = [keep_local(packs.at[a, group[a]], packs_in.at[a, group[a]], local.at[a]) for a in range(2)]
    own_l = [keep_local(table.at[a, group[a]], table_in.at[a, group[a]], local.at[2 + a]) for a in range(2)]
    l_copies = [[], []]

    def send_table(ks):
        for k in ks:
            for a in range(2):
                p = to[a][k]
                l_copies[a].append(
                    remote(table.at[a, p], table_in.at[a, group[a]], l_send.at[a, k], l_recv.at[a, k], peer(a, p))
                )

    send_table(TABLE_STEPS[0])

    pairs = waves.shape[1]
    per = pairs // RING
    wave_row = waves[...].astype(jnp.float32)

    def waves_of(slot):
        lanes = lax.broadcasted_iota(jnp.int32, (slot.shape[0], pairs), 1)
        return jnp.sum(jnp.where(lanes == slot, wave_row, 0.0), axis=1, keepdims=True)

    row = lax.broadcasted_iota(jnp.int32, (6 * RING * RING, 1), 0)
    block, inner = row // (RING * RING), lax.rem(row, RING * RING)
    part, member = block // 3, lax.rem(block, 3)
    slot = jnp.minimum(part * 3 * RING + lax.rem(inner, RING) * 3 + member, per - 1)
    found = waves_of((inner // RING) * per + slot)
    orders[...] = jnp.broadcast_to(found, orders.shape)

    lane = lax.broadcasted_iota(jnp.int32, (1, 128), 1).astype(jnp.float32)

    def make_basis(block):
        u = orders[pl.ds(pl.multiple_of(block * 64, 64), 64), :]
        half = jnp.floor(u * 0.5) * 2.0
        even = jnp.where(half == u, u, (HALF - 1.0) - u)
        for par in range(2):
            order = even if par == 0 else (HALF - 1.0) - even
            weight = jnp.where(order == 0.0, 1.0, 2.0)
            cos, sin = turn(order * lane)
            cos, sin = weight * cos, weight * sin
            cos_t, sin_t = turn(order * (lane * 128.0))
            for t in range(6):
                ct, st = cos_t[:, t : t + 1], sin_t[:, t : t + 1]
                for e, value in enumerate((cos * ct - sin * st, -(sin * ct + cos * st))):
                    hi, lo = split_bf16(value)
                    for j, item in enumerate((hi, hi, lo)):
                        basis[par, block, pl.ds(j * 128 + e * 64, 64), pl.ds(t * 128, 128)] = item

    def make_bases(start, count):
        lax.fori_loop(start, start + count, lambda n, c: (make_basis(n), c)[1], 0)

    column = lax.broadcasted_iota(jnp.int32, (1, table.shape[3]), 1)
    deg_dev = packs.shape[2] // 4
    deg = RING * deg_dev
    turned_column = (
        lax.rem(column, deg) // deg_dev * deg + column // deg * deg_dev + lax.rem(column, deg_dev)
    )
    natural = lax.broadcasted_iota(jnp.int32, perm.shape, 0)
    perm[...] = jnp.where(natural == turned_column, 1.0, 0.0).astype(jnp.bfloat16)
    made = 0
    make_bases(made, BASIS_STEPS[0])
    made += BASIS_STEPS[0]

    def ring_send(a, dirn, step, s):
        org = lax.rem(place[a] + (RING - step if dirn == 0 else step), RING)
        ref = coef_all.at[a, org, pl.ds(s * (deg // 2), deg // 2)]
        return remote(ref, ref, r_send.at[a, dirn, step, s], r_recv.at[a, dirn, step, s], next_to[a][dirn])

    def hops(dirn, s):
        return 4 if s == dirn else 3

    live = {}
    for a in range(2):
        own_c[a].wait()
        for copy in c_copies[a]:
            copy.wait_recv()
        wide[a] = packs_in[a].astype(jnp.float32)
        for s in range(RING):
            for t in range(4):
                piece = wide[a, s, pl.ds(t * deg_dev, deg_dev), :]
                coef_rows[a, pl.ds(s * deg_dev, deg_dev), pl.ds(t * 128, 128)] = piece
        coef_all[a, place[a]] = coef_rows[a].astype(jnp.bfloat16)
        for s in range(2):
            for dirn in range(2):
                live[a, dirn, 0, s] = ring_send(a, dirn, 0, s)
    for step in range(1, 5):
        if step < 4:
            send_table(TABLE_STEPS[step])
            if BASIS_STEPS[step]:
                make_bases(made, BASIS_STEPS[step])
                made += BASIS_STEPS[step]
        for a in range(2):
            for s in range(2):
                for dirn in range(2):
                    if step <= hops(dirn, s):
                        live[a, dirn, step - 1, s].wait_recv()
                        if step < hops(dirn, s):
                            live[a, dirn, step, s] = ring_send(a, dirn, step, s)

    row = lax.broadcasted_iota(jnp.int32, (32, 1), 0)
    member = jnp.minimum(jnp.where(row < 24, row // 8, (row - 24) // 2), 2)
    lane_in = lax.rem(lax.broadcasted_iota(jnp.int32, (1, 1, 512), 2), 256)
    lane_out = lax.broadcasted_iota(jnp.int32, (1, 1, 128), 2)

    def make_coded(a):
        own_l[a].wait()
        for copy in l_copies[a]:
            copy.wait_recv()
        u = waves_of(ma * per + jnp.minimum(a * 3 * RING + group[a] * 3 + member, per - 1))
        cut = HALF - u
        even = jnp.floor(u * 0.5) * 2.0 == u
        bounds = (
            (jnp.where(even, 0.0, cut), jnp.where(even, cut, HALF + 1.0)),
            (jnp.where(even, cut, 0.0), jnp.where(even, HALF + 1.0, cut)),
        )
        if a == 0:
            rows_a = table_in[0].astype(jnp.float32)
            at = column
        else:
            flat = table_in[1].reshape(RING * 32, -1)
            rows_a = jnp.dot(flat, perm[...], preferred_element_type=jnp.float32).reshape(RING, 32, -1)
            at = turned_column
        at = at.astype(jnp.float32)
        rhs = coef_all[a].reshape(-1, 512)
        for par in range(2):
            low, high = bounds[par]
            keep = ((at >= low) & (at < high))[None]
            lhs = jnp.where(keep, rows_a, 0.0).astype(jnp.bfloat16).reshape(RING * 32, -1)
            sums = jnp.dot(lhs, rhs, preferred_element_type=jnp.float32)
            sums = sums.reshape(RING, 4, 8, 512)
            tail = sums[:, 3]
            two, four = pltpu.roll(tail, 6, 1), pltpu.roll(tail, 4, 1)
            parts = (
                (0, 8, (sums[:, 0], sums[:, 1], sums[:, 2])),
                (8, 2, (tail, two, four)),
            )
            for start, count, (s0, s1, s2) in parts:
                value = jnp.where(lane_in < CH, s0, jnp.where(lane_in < 2 * CH, s1, s2))
                value = jnp.where(lane_in < 3 * CH, value, 0.0)
                top = jnp.max(jnp.abs(value), axis=2, keepdims=True)
                power = jnp.ceil(jnp.log2(jnp.maximum(top, 1e-30)) + 1e-3)
                code = jnp.round(value * (jnp.exp2(-power) * 32767.0)).astype(jnp.int32)
                word = (code[:, :, :256] << 16) | (code[:, :, 256:] & 0xFFFF)
                first, second = word[:, :, :128], word[:, :, 128:]
                second = jnp.where(lane_out == 3 * CH - 128, power.astype(jnp.int32), second)
                for half, item in enumerate((first, second)):
                    coded[a, :, start : start + count, par * 2 + half, :] = item[:, :count]

    b_copies = [[], []]
    m_copies = [[], []]
    own_m = [[], []]

    def forward(a, k, src, sent):
        for j, p in enumerate(ma_to):
            m_copies[a].append(
                remote(
                    src.at[pl.ds((5 * p) // 4, 2)], words.at[a, ma, sent],
                    m_send.at[a, k, j], m_recv.at[a, k, j], (lat, p),
                )
            )
        own_m[a].append(
            keep_local(src.at[pl.ds((5 * ma) // 4, 2)], words.at[a, ma, sent], local.at[4 + 8 * a + k])
        )

    def send_coded(a):
        for k in range(7):
            p = to[a][k]
            b_copies[a].append(
                remote(coded.at[a, p], back.at[a, group[a]], b_send.at[a, k], b_recv.at[a, k], peer(a, p))
            )
        forward(a, 7, coded.at[a, group[a]], group[a])

    def forward_all(a):
        for k in range(7):
            b_copies[a][k].wait_recv()
            forward(a, k, back.at[a, source[a][k]], source[a][k])

    def synthesize(a):
        for copy in own_m[a]:
            copy.wait()
        for copy in m_copies[a]:
            copy.wait_recv()
        for par in range(2):
            for i in range(2):
                first = words[a, :, :, i, par * 2, :].reshape(64, 128)
                second = words[a, :, :, i, par * 2 + 1, :].reshape(64, 128)
                power = second[:, 3 * CH - 128 : 3 * CH - 127].astype(jnp.float32)
                scale = jnp.exp2(power) * (1.0 / 32767.0)
                for half, word in enumerate((first, second)):
                    real = (word >> 16).astype(jnp.float32) * scale
                    imag = ((word << 16) >> 16).astype(jnp.float32) * scale
                    both = jnp.concatenate([real, imag], axis=0)
                    turned[pl.ds(half * 128, 128), :] = both.T
                for b in range(3):
                    hi, lo = split_bf16(turned[pl.ds(b * CH, 96), :])
                    for j, item in enumerate((hi, lo, hi)):
                        rows[par, pl.ds(i * 96, 96), pl.ds((b * 3 + j) * 128, 128)] = item
            term = jnp.dot(
                rows[par], basis[par, 3 * a : 3 * a + 3].reshape(1152, -1), preferred_element_type=jnp.float32
            )
            if a == 0:
                total[par] = term
            else:
                total[par] += term

    turned[pl.ds(256, turned.shape[0] - 256), :] = jnp.zeros((turned.shape[0] - 256, 128), jnp.float32)
    make_coded(0)
    send_coded(0)
    make_coded(1)
    send_coded(1)
    forward_all(0)
    forward_all(1)
    synthesize(0)
    synthesize(1)

    edge = HALF - 640
    lanes = lax.broadcasted_iota(jnp.int32, (1, 128), 1)
    for i in range(2):
        even, odd = total[0, pl.ds(i * 96, CH), :], total[1, pl.ds(i * 96, CH), :]
        plus = even + odd
        minus = pltpu.roll(even - odd, edge, 1)
        at = pl.ds(i * CH, CH)
        out[at, :640] = plus[:, :640]
        out[at, 640:768] = jnp.where(lanes < edge, plus[:, 640:], minus[:, :128])
        out[at, 768:1408] = minus[:, 128:]
        out[at, 1408:] = minus[:, : LON - 1408]

    for a in range(2):
        for copy in c_copies[a] + l_copies[a] + b_copies[a] + m_copies[a]:
            copy.wait_send()
    for copy in live.values():
        copy.wait_send()


def synth_call(waves, table, packs):
    vmem = pl.BlockSpec(memory_space=pltpu.VMEM)
    dma = pltpu.SemaphoreType.DMA
    deg = packs.shape[2] // 4 * RING
    deg_all = table.shape[3]
    f32, bf16, s32 = jnp.float32, jnp.bfloat16, jnp.int32
    return pl.pallas_call(
        synth_kernel,
        out_shape=jax.ShapeDtypeStruct((2 * CH, LON), f32),
        in_specs=[vmem, vmem, vmem],
        out_specs=vmem,
        scratch_shapes=[
            pltpu.VMEM(table.shape, bf16),
            pltpu.VMEM(packs.shape, bf16),
            pltpu.VMEM(packs.shape, f32),
            pltpu.VMEM((2, deg, 512), f32),
            pltpu.VMEM((2, RING, deg, 512), bf16),
            pltpu.VMEM((2, RING, 10, 4, 128), s32),
            pltpu.VMEM((2, RING, 10, 4, 128), s32),
            pltpu.VMEM((2, RING, RING, 2, 4, 128), s32),
            pltpu.VMEM((deg_all, deg_all), bf16),
            pltpu.VMEM((6 * 64, 128), f32),
            pltpu.VMEM((2, 6, 384, 768), bf16),
            pltpu.VMEM((272, 128), f32),
            pltpu.VMEM((2, 192, 1152), bf16),
            pltpu.VMEM((2, 192, 768), f32),
            dma((2, 7)), dma((2, 7)), dma((2, 7)), dma((2, 7)),
            dma((2, 2, 4, 2)), dma((2, 2, 4, 2)),
            dma((2, 7)), dma((2, 7)), dma((2, 8, 7)), dma((2, 8, 7)), dma((20,)),
        ],
        compiler_params=pltpu.CompilerParams(
            collective_id=0, has_side_effects=True, vmem_limit_bytes=48 << 20
        ),
        name="synth",
    )(waves, table, packs)


def body(pair_wave, legendre, coefs):
    ma_i = lax.axis_index("ma")
    table, packs = pack_table(legendre), pack_coefs(coefs)
    both = synth_call(pair_wave.reshape(1, -1), table, packs)
    start = 105 * ma_i - CH * ((5 * ma_i) // 4)
    return lax.dynamic_slice_in_dim(both, start, 105, axis=0)


def solution(mesh):
    in_specs = (P(), P("ma", "lat", None), P("ma", "lat", None))
    out_specs = P(("lat", "ma"), None)
    return jax.shard_map(body, mesh=mesh, in_specs=in_specs, out_specs=out_specs, check_vma=False)
```

```python
import math

import jax
import jax.numpy as jnp
from jax import lax
from jax.experimental import pallas as pl
from jax.experimental.pallas import tpu as pltpu
from jax.sharding import PartitionSpec as P

LON = 1440
HALF = 720
RING = 8
ORDER = (1, 7, 2, 6, 3, 5, 4)
TABLE_STEPS = ((4, 5), (2, 3), (6,), (0, 1))
BASIS_STEPS = (3, 2, 1, 0)
CH = 84
SINE = [(-1.0) ** n / math.factorial(2 * n + 1) for n in range(6)]
COSINE = [(-1.0) ** n / math.factorial(2 * n) for n in range(7)]
MESH = pl.DeviceIdType.MESH


def pack_table(legendre):
    slots, rows_dev, row_count = legendre.shape
    table = jnp.pad(legendre, ((0, 6 * RING - slots), (0, 0), (0, 0)))
    head = table[:, :8].reshape(2, RING, 24, row_count)
    tail = table[:, 8:].reshape(2, RING, 6, row_count)
    tail = jnp.pad(tail, ((0, 0), (0, 0), (0, 2), (0, 0)))
    return jnp.concatenate([head, tail], axis=2)


def pack_coefs(coefs):
    slots, deg_dev, cols = coefs.shape
    x = jnp.pad(coefs, ((0, 6 * RING - slots), (0, 0), (0, 0)))
    x = x.reshape(2, RING, 3, deg_dev, 2, CH).transpose(0, 1, 4, 3, 2, 5)
    x = x.reshape(2, RING, 2, deg_dev, 3 * CH)
    x = jnp.pad(x, ((0, 0),) * 4 + ((0, 256 - 3 * CH),))
    x = x.reshape(2, RING, 2, deg_dev, 2, 128).transpose(0, 1, 2, 4, 3, 5)
    return x.reshape(2, RING, 4 * deg_dev, 128)


def poly(coefficients, square):
    value = jnp.float32(coefficients[-1])
    for coefficient in coefficients[-2::-1]:
        value = value * square + coefficient
    return value


def turn(phase):
    turns = jnp.round(phase * (1.0 / LON))
    angle = (phase - turns * LON) * (math.pi / LON)
    square = angle * angle
    sine = angle * poly(SINE, square)
    return 1.0 - 2.0 * (sine * sine), 2.0 * (sine * poly(COSINE, square))


def split_bf16(x):
    hi = x.astype(jnp.bfloat16)
    return hi, (x - hi.astype(jnp.float32)).astype(jnp.bfloat16)


def synth_kernel(
    waves, table, packs, out,
    table_in, packs_in, wide, coef_rows, coef_all, raw, coded, back, words,
    perm, orders, basis, turned, blocks, rows, total,
    c_send, c_recv, l_send, l_recv, r_send, r_recv,
    b_send, b_recv, m_send, m_recv, own_sem,
):
    lat = lax.axis_index("lat")
    ma = lax.axis_index("ma")
    y = lat // RING
    z = lax.rem(lat, RING)
    group = (z, y)
    place = (y, z)
    to = [[lax.rem(group[a] + d, RING) for d in ORDER] for a in range(2)]
    ma_to = [lax.rem(ma + d, RING) for d in ORDER]

    def peer(a, p):
        return (y * RING + p, ma) if a == 0 else (p * RING + z, ma)

    next_to = [
        [peer(1 - a, lax.rem(place[a] + step, RING)) for step in (1, RING - 1)]
        for a in range(2)
    ]

    barrier = pltpu.get_barrier_semaphore()
    targets = [peer(a, p) for a in range(2) for p in to[a]] + [(lat, p) for p in ma_to]
    for target in targets:
        pl.semaphore_signal(barrier, inc=1, device_id=target, device_id_type=MESH)
    pl.semaphore_wait(barrier, len(targets))

    def remote(src, dst, send, recv, target):
        copy = pltpu.make_async_remote_copy(
            src_ref=src, dst_ref=dst, send_sem=send, recv_sem=recv,
            device_id=target, device_id_type=MESH,
        )
        copy.start()
        return copy

    def keep_local(src, dst, sem):
        copy = pltpu.make_async_copy(src, dst, sem)
        copy.start()
        return copy

    def wait_bytes(ref, sem):
        pltpu.make_async_copy(ref, ref, sem).wait()

    for k in range(6, -1, -1):
        for a in range(2):
            p = to[a][k]
            remote(packs.at[a, p], packs_in.at[a, group[a]], c_send.at[a], c_recv.at[a], peer(a, p))
    own_c = [keep_local(packs.at[a, group[a]], packs_in.at[a, group[a]], own_sem.at[0, a]) for a in range(2)]
    own_l = [keep_local(table.at[a, group[a]], table_in.at[a, group[a]], own_sem.at[1, a]) for a in range(2)]

    def send_table(ks):
        for k in ks:
            for a in range(2):
                p = to[a][k]
                remote(table.at[a, p], table_in.at[a, group[a]], l_send.at[a], l_recv.at[a], peer(a, p))

    send_table(TABLE_STEPS[0])

    pairs = waves.shape[1]
    per = pairs // RING
    wave_row = waves[...].astype(jnp.float32)

    def waves_of(slot):
        lanes = lax.broadcasted_iota(jnp.int32, (slot.shape[0], pairs), 1)
        return jnp.sum(jnp.where(lanes == slot, wave_row, 0.0), axis=1, keepdims=True)

    row = lax.broadcasted_iota(jnp.int32, (6 * RING * RING, 1), 0)
    block, inner = row // (RING * RING), lax.rem(row, RING * RING)
    part, member = block // 3, lax.rem(block, 3)
    near = lax.rem(inner, RING)
    step = jnp.where(lax.rem(near, 2) == 1, (near + 1) // 2, RING - near // 2)
    came = lax.rem(jnp.where(part == 0, group[0], group[1]) + RING - step, RING)
    slot = jnp.minimum(part * 3 * RING + came * 3 + member, per - 1)
    found = waves_of((inner // RING) * per + slot)
    orders[...] = jnp.broadcast_to(found, orders.shape)

    lane = lax.broadcasted_iota(jnp.int32, (1, 128), 1).astype(jnp.float32)

    def make_basis(block):
        u = orders[pl.ds(pl.multiple_of(block * 64, 64), 64), :]
        half = jnp.floor(u * 0.5) * 2.0
        even = jnp.where(half == u, u, (HALF - 1.0) - u)
        for par in range(2):
            order = even if par == 0 else (HALF - 1.0) - even
            weight = jnp.where(order == 0.0, 1.0, 2.0)
            cos, sin = turn(order * lane)
            cos, sin = weight * cos, weight * sin
            cos_t, sin_t = turn(order * (lane * 128.0))
            for t in range(6):
                ct, st = cos_t[:, t : t + 1], sin_t[:, t : t + 1]
                for e, value in enumerate((cos * ct - sin * st, -(sin * ct + cos * st))):
                    hi, lo = split_bf16(value)
                    for j, item in enumerate((hi, hi, lo)):
                        basis[par, block, pl.ds(j * 128 + e * 64, 64), pl.ds(t * 128, 128)] = item

    def make_bases(start, count):
        lax.fori_loop(start, start + count, lambda n, c: (make_basis(n), c)[1], 0)

    column = lax.broadcasted_iota(jnp.int32, (1, table.shape[3]), 1)
    deg_dev = packs.shape[2] // 4
    deg = RING * deg_dev
    turned_column = (
        lax.rem(column, deg) // deg_dev * deg + column // deg * deg_dev + lax.rem(column, deg_dev)
    )
    natural = lax.broadcasted_iota(jnp.int32, perm.shape, 0)
    perm[...] = jnp.where(natural == turned_column, 1.0, 0.0).astype(jnp.bfloat16)
    made = 0
    make_bases(made, BASIS_STEPS[0])
    made += BASIS_STEPS[0]

    def ring_send(a, dirn, step, s):
        org = lax.rem(place[a] + (RING - step if dirn == 0 else step), RING)
        ref = coef_all.at[a, org, pl.ds(s * (deg // 2), deg // 2)]
        return remote(ref, ref, r_send.at[a], r_recv.at[a, dirn, step, s], next_to[a][dirn])

    def hops(dirn, s):
        return 4 if s == dirn else 3

    live = {}
    for a in range(2):
        own_c[a].wait()
        wait_bytes(packs_in.at[a, pl.ds(0, 7)], c_recv.at[a])
        wide[a] = packs_in[a].astype(jnp.float32)
        for s in range(RING):
            for t in range(4):
                piece = wide[a, s, pl.ds(t * deg_dev, deg_dev), :]
                coef_rows[a, pl.ds(s * deg_dev, deg_dev), pl.ds(t * 128, 128)] = piece
        coef_all[a, place[a]] = coef_rows[a].astype(jnp.bfloat16)
        for s in range(2):
            for dirn in range(2):
                live[a, dirn, 0, s] = ring_send(a, dirn, 0, s)

    def ring_step(a, step):
        for s in range(2):
            for dirn in range(2):
                if step <= hops(dirn, s):
                    live[a, dirn, step - 1, s].wait_recv()
                    if step < hops(dirn, s):
                        live[a, dirn, step, s] = ring_send(a, dirn, step, s)

    for step in range(1, 4):
        send_table(TABLE_STEPS[step])
        if BASIS_STEPS[step]:
            make_bases(made, BASIS_STEPS[step])
            made += BASIS_STEPS[step]
        for a in range(2):
            ring_step(a, step)

    row = lax.broadcasted_iota(jnp.int32, (32, 1), 0)
    member = jnp.minimum(jnp.where(row < 24, row // 8, (row - 24) // 2), 2)
    lane_in = lax.rem(lax.broadcasted_iota(jnp.int32, (1, 1, 512), 2), 256)
    lane_out = lax.broadcasted_iota(jnp.int32, (1, 256), 1)
    lane_left = lax.broadcasted_iota(jnp.int32, (1, 128), 1)

    def make_coded(a):
        ring_step(a, 4)
        own_l[a].wait()
        wait_bytes(table_in.at[a, pl.ds(0, 7)], l_recv.at[a])
        u = waves_of(ma * per + jnp.minimum(a * 3 * RING + group[a] * 3 + member, per - 1))
        cut = HALF - u
        even = jnp.floor(u * 0.5) * 2.0 == u
        bounds = (
            (jnp.where(even, 0.0, cut), jnp.where(even, cut, HALF + 1.0)),
            (jnp.where(even, cut, 0.0), jnp.where(even, HALF + 1.0, cut)),
        )
        if a == 0:
            rows_a = table_in[0].astype(jnp.float32)
            at = column
        else:
            flat = table_in[1].reshape(RING * 32, -1)
            rows_a = jnp.dot(flat, perm[...], preferred_element_type=jnp.float32).reshape(RING, 32, -1)
            at = turned_column
        at = at.astype(jnp.float32)
        rhs = coef_all[a].reshape(-1, 512)
        for par in range(2):
            low, high = bounds[par]
            keep = ((at >= low) & (at < high))[None]
            lhs = jnp.where(keep, rows_a, 0.0).astype(jnp.bfloat16).reshape(RING * 32, -1)
            sums = jnp.dot(lhs, rhs, preferred_element_type=jnp.float32)
            sums = sums.reshape(RING, 4, 8, 512)
            tail = sums[:, 3]
            two, four = pltpu.roll(tail, 6, 1), pltpu.roll(tail, 4, 1)
            parts = (
                (0, 8, (sums[:, 0], sums[:, 1], sums[:, 2])),
                (8, 2, (tail, two, four)),
            )
            for start, count, (s0, s1, s2) in parts:
                value = jnp.where(lane_in < CH, s0, jnp.where(lane_in < 2 * CH, s1, s2))
                value = jnp.where(lane_in < 3 * CH, value, 0.0)
                top = jnp.max(jnp.abs(value), axis=2, keepdims=True)
                power = jnp.ceil(jnp.log2(jnp.maximum(top, 1e-30)) + 1e-3)
                code = jnp.round(value * (jnp.exp2(-power) * 32767.0)).astype(jnp.int32)
                word = (code[:, :, :256] << 16) | (code[:, :, 256:] & 0xFFFF)
                word = jnp.where(lane_in[:, :, :256] < 3 * CH, word, power.astype(jnp.int32))
                raw[par, :, start : start + count, :] = word[:, :count]
        for p in range(RING):
            i0, cut = (5 * p) // 4, 21 * (p % 4)
            left = None
            for par in range(2):
                one, two = raw[par, :, i0, :], raw[par, :, i0 + 1, :]
                main = one
                if cut:
                    near = pltpu.roll(one, 256 - cut, 1)
                    main = jnp.where(lax.rem(lane_out, CH) < CH - cut, near, pltpu.roll(two, CH - cut, 1))
                main = jnp.where(lane_out < 3 * CH, main, jnp.where(lane_out == 3 * CH, one, two))
                for half in range(2):
                    coded[a, :, p * 5 + par * 2 + half, 0, :] = main[:, half * 128 : half * 128 + 128]
                for b in range(3):
                    shift = 63 * par - 63 * b - cut
                    item = (pltpu.roll(two, shift % 256, 1) if shift else two)[:, :128]
                    left = item if left is None else jnp.where(lane_left < 63 * par + 21 * b, left, item)
            coded[a, :, p * 5 + 4, 0, :] = left

    own_b = []
    own_m = []

    def send_coded(a):
        own_b.append(keep_local(coded.at[a, group[a]], back.at[a, 0], own_sem.at[2, a]))
        for k in range(7):
            p = to[a][k]
            remote(coded.at[a, p], back.at[a, k + 1], b_send.at[a], b_recv.at[a, (k + 1) // 4], peer(a, p))

    def forward(a, batch):
        if batch == 0:
            own_b[a].wait()
            wait_bytes(back.at[a, pl.ds(1, 3)], b_recv.at[a, 0])
        else:
            wait_bytes(back.at[a, pl.ds(4, 4)], b_recv.at[a, 1])
        four = pl.ds(4 * batch, 4)
        for p in ma_to:
            remote(
                back.at[a, four, pl.ds(5 * p, 5)], words.at[a, ma, four],
                m_send.at[a], m_recv.at[a], (lat, p),
            )
        own_m.append(keep_local(back.at[a, four, pl.ds(5 * ma, 5)], words.at[a, ma, four], own_sem.at[3 + batch, a]))

    limit = CH - 21 * lax.rem(ma, 4)

    def plane(a, k):
        return words[a, :, :, k, 0, :].reshape(64, 128)

    def unit(power):
        return jnp.exp2(power.astype(jnp.float32)) * (1.0 / 32767.0)

    def turned_rows(word, scale):
        real = (word >> 16).astype(jnp.float32) * scale
        imag = ((word << 16) >> 16).astype(jnp.float32) * scale
        return jnp.concatenate([real, imag], axis=0).T

    def synthesize(a):
        wait_bytes(words.at[a, pl.ds(0, 7)], m_recv.at[a])
        scales = []
        for par in range(2):
            first, second = plane(a, par * 2), plane(a, par * 2 + 1)
            scale0 = unit(second[:, 3 * CH - 128 : 3 * CH - 127])
            scale1 = unit(second[:, 3 * CH - 127 : 3 * CH - 126])
            scales.append(scale1)
            for half, word in enumerate((first, second)):
                scale = jnp.where(lax.rem(lane_left + half * 128, CH) < limit, scale0, scale1)
                turned[par, pl.ds(half * 128, 128), :] = turned_rows(word, scale)
        turned[2, pl.ds(0, 128), :] = turned_rows(plane(a, 4), jnp.where(lane_left < 63, scales[0], scales[1]))
        for par in range(2):
            for b in range(3):
                blocks[par, b, pl.ds(0, CH), :] = turned[par, pl.ds(b * CH, CH), :]
                blocks[par, b, pl.ds(CH, 21), :] = turned[2, pl.ds(63 * par + 21 * b, 21), :]
                hi, lo = split_bf16(blocks[par, b])
                for j, item in enumerate((hi, lo, hi)):
                    rows[par, :, pl.ds((b * 3 + j) * 128, 128)] = item
            term = jnp.dot(
                rows[par], basis[par, 3 * a : 3 * a + 3].reshape(1152, -1), preferred_element_type=jnp.float32
            )
            if a == 0:
                total[par] = term
            else:
                total[par] += term

    blocks[...] = jnp.zeros(blocks.shape, jnp.float32)
    make_coded(0)
    send_coded(0)
    make_coded(1)
    send_coded(1)
    for batch in range(2):
        for a in range(2):
            forward(a, batch)
    for copy in own_m:
        copy.wait()
    synthesize(0)
    synthesize(1)

    edge = HALF - 640
    even, odd = total[0], total[1]
    plus = even + odd
    minus = pltpu.roll(even - odd, edge, 1)
    count = out.shape[0]
    out[:, :640] = plus[:count, :640]
    out[:, 640:768] = jnp.where(lane_left < edge, plus[:, 640:], minus[:, :128])[:count]
    out[:, 768:1408] = minus[:count, 128:]
    out[:, 1408:] = minus[:count, : LON - 1408]

    seven = pl.ds(0, 7)
    for a in range(2):
        wait_bytes(packs_in.at[a, seven], c_send.at[a])
        wait_bytes(table_in.at[a, seven], l_send.at[a])
        wait_bytes(coef_all.at[a, seven], r_send.at[a])
        wait_bytes(back.at[a, seven], b_send.at[a])
        wait_bytes(words.at[a, seven], m_send.at[a])


def synth_call(waves, table, packs):
    vmem = pl.BlockSpec(memory_space=pltpu.VMEM)
    dma = pltpu.SemaphoreType.DMA
    deg = packs.shape[2] // 4 * RING
    deg_all = table.shape[3]
    f32, bf16, s32 = jnp.float32, jnp.bfloat16, jnp.int32
    return pl.pallas_call(
        synth_kernel,
        out_shape=jax.ShapeDtypeStruct((105, LON), f32),
        in_specs=[vmem, vmem, vmem],
        out_specs=vmem,
        scratch_shapes=[
            pltpu.VMEM(table.shape, bf16),
            pltpu.VMEM(packs.shape, bf16),
            pltpu.VMEM(packs.shape, f32),
            pltpu.VMEM((2, deg, 512), f32),
            pltpu.VMEM((2, RING, deg, 512), bf16),
            pltpu.VMEM((2, RING, 10, 256), s32),
            pltpu.VMEM((2, RING, 5 * RING, 1, 128), s32),
            pltpu.VMEM((2, RING, 5 * RING, 1, 128), s32),
            pltpu.VMEM((2, RING, RING, 5, 1, 128), s32),
            pltpu.VMEM((deg_all, deg_all), bf16),
            pltpu.VMEM((6 * 64, 128), f32),
            pltpu.VMEM((2, 6, 384, 768), bf16),
            pltpu.VMEM((3, 256, 128), f32),
            pltpu.VMEM((2, 3, 112, 128), f32),
            pltpu.VMEM((2, 112, 1152), bf16),
            pltpu.VMEM((2, 112, 768), f32),
            dma((2,)), dma((2,)), dma((2,)), dma((2,)),
            dma((2,)), dma((2, 2, 4, 2)),
            dma((2,)), dma((2, 2)), dma((2,)), dma((2,)), dma((5, 2)),
        ],
        compiler_params=pltpu.CompilerParams(
            collective_id=0, has_side_effects=True, vmem_limit_bytes=48 << 20
        ),
        name="synth",
    )(waves, table, packs)


def body(pair_wave, legendre, coefs):
    table, packs = pack_table(legendre), pack_coefs(coefs)
    return synth_call(pair_wave.reshape(1, -1), table, packs)


def solution(mesh):
    in_specs = (P(), P("ma", "lat", None), P("ma", "lat", None))
    out_specs = P(("lat", "ma"), None)
    return jax.shard_map(body, mesh=mesh, in_specs=in_specs, out_specs=out_specs, check_vma=False)
```

```python
import math

import jax
import jax.numpy as jnp
from jax import lax
from jax.experimental import pallas as pl
from jax.experimental.pallas import tpu as pltpu
from jax.sharding import PartitionSpec as P

LON = 1440
HALF = 720
RING = 8
ORDER = (1, 7, 2, 6, 3, 5, 4)
TABLE_STEPS = ((4, 5), (2, 3), (6,), (0, 1))
BASIS_STEPS = (3, 2, 1, 0)
CH = 84
SINE = [(-1.0) ** n / math.factorial(2 * n + 1) for n in range(6)]
COSINE = [(-1.0) ** n / math.factorial(2 * n) for n in range(7)]
MESH = pl.DeviceIdType.MESH


def pack_coefs(coefs):
    slots, deg_dev, cols = coefs.shape
    x = jnp.pad(coefs, ((0, 6 * RING - slots), (0, 0), (0, 0)))
    x = x.reshape(2, RING, 3, deg_dev, 2, CH).transpose(0, 1, 4, 3, 2, 5)
    x = x.reshape(2, RING, 2, deg_dev, 3 * CH)
    x = jnp.pad(x, ((0, 0),) * 4 + ((0, 256 - 3 * CH),))
    x = x.reshape(2, RING, 2, deg_dev, 2, 128).transpose(0, 1, 2, 4, 3, 5)
    return x.reshape(2, RING, 4 * deg_dev, 128)


def poly(coefficients, square):
    value = jnp.float32(coefficients[-1])
    for coefficient in coefficients[-2::-1]:
        value = value * square + coefficient
    return value


def turn(phase):
    turns = jnp.round(phase * (1.0 / LON))
    angle = (phase - turns * LON) * (math.pi / LON)
    square = angle * angle
    sine = angle * poly(SINE, square)
    return 1.0 - 2.0 * (sine * sine), 2.0 * (sine * poly(COSINE, square))


def split_bf16(x):
    hi = x.astype(jnp.bfloat16)
    return hi, (x - hi.astype(jnp.float32)).astype(jnp.bfloat16)


def synth_kernel(
    waves, tables, packs, out,
    table_raw, table_flat, pick, table, table_in, packs_in, wide, coef_rows, coef_all, raw, coded, back, words,
    perm, orders, basis, turned, blocks, rows, total,
    c_send, c_recv, l_send, l_recv, r_send, r_recv,
    b_send, b_recv, m_send, m_recv, own_sem,
):
    lat = lax.axis_index("lat")
    ma = lax.axis_index("ma")
    y = lat // RING
    z = lax.rem(lat, RING)
    group = (z, y)
    place = (y, z)
    to = [[lax.rem(group[a] + d, RING) for d in ORDER] for a in range(2)]
    ma_to = [lax.rem(ma + d, RING) for d in ORDER]

    def peer(a, p):
        return (y * RING + p, ma) if a == 0 else (p * RING + z, ma)

    next_to = [
        [peer(1 - a, lax.rem(place[a] + step, RING)) for step in (1, RING - 1)]
        for a in range(2)
    ]

    load = pltpu.make_async_copy(tables, table_raw, own_sem.at[5, 0])
    load.start()
    barrier = pltpu.get_barrier_semaphore()
    targets = [peer(a, p) for a in range(2) for p in to[a]] + [(lat, p) for p in ma_to]
    for target in targets:
        pl.semaphore_signal(barrier, inc=1, device_id=target, device_id_type=MESH)
    pl.semaphore_wait(barrier, len(targets))

    def remote(src, dst, send, recv, target):
        copy = pltpu.make_async_remote_copy(
            src_ref=src, dst_ref=dst, send_sem=send, recv_sem=recv,
            device_id=target, device_id_type=MESH,
        )
        copy.start()
        return copy

    def keep_local(src, dst, sem):
        copy = pltpu.make_async_copy(src, dst, sem)
        copy.start()
        return copy

    def wait_bytes(ref, sem):
        pltpu.make_async_copy(ref, ref, sem).wait()

    for k in range(6, -1, -1):
        for a in range(2):
            p = to[a][k]
            remote(packs.at[a, p], packs_in.at[a, group[a]], c_send.at[a], c_recv.at[a], peer(a, p))
    own_c = [keep_local(packs.at[a, group[a]], packs_in.at[a, group[a]], own_sem.at[0, a]) for a in range(2)]

    lats, slots, deg_all = tables.shape
    stride = 48
    table_flat[...] = jnp.zeros(table_flat.shape, table_flat.dtype)
    row = lax.broadcasted_iota(jnp.int32, (RING * 32, 1), 0)
    inner = lax.rem(row, 32)
    member = jnp.where(inner < 24, inner // 8, (inner - 24) // 2)
    at_lat = jnp.where(inner < 24, lax.rem(inner, 8), 8 + lax.rem(inner, 2))
    for a in range(2):
        want = at_lat * stride + a * 3 * RING + row // 32 * 3 + member
        want = jnp.where(inner < 30, want, -1)
        lanes = lax.broadcasted_iota(jnp.int32, (RING * 32, lats * stride), 1)
        pick[a] = jnp.where(lanes == want, 1.0, 0.0).astype(jnp.bfloat16)
    load.wait()
    for i in range(lats):
        table_flat[pl.ds(i * stride, slots), :] = table_raw[i]
    for a in range(2):
        moved = jnp.dot(pick[a], table_flat[...], preferred_element_type=jnp.float32)
        table[a] = moved.astype(jnp.bfloat16).reshape(RING, 32, deg_all)
    own_l = [keep_local(table.at[a, group[a]], table_in.at[a, group[a]], own_sem.at[1, a]) for a in range(2)]

    def send_table(ks):
        for k in ks:
            for a in range(2):
                p = to[a][k]
                remote(table.at[a, p], table_in.at[a, group[a]], l_send.at[a], l_recv.at[a], peer(a, p))

    send_table(TABLE_STEPS[0])

    pairs = waves.shape[1]
    per = pairs // RING
    wave_row = waves[...].astype(jnp.float32)

    def waves_of(slot):
        lanes = lax.broadcasted_iota(jnp.int32, (slot.shape[0], pairs), 1)
        return jnp.sum(jnp.where(lanes == slot, wave_row, 0.0), axis=1, keepdims=True)

    row = lax.broadcasted_iota(jnp.int32, (6 * RING * RING, 1), 0)
    block, inner = row // (RING * RING), lax.rem(row, RING * RING)
    part, member = block // 3, lax.rem(block, 3)
    near = lax.rem(inner, RING)
    step = jnp.where(lax.rem(near, 2) == 1, (near + 1) // 2, RING - near // 2)
    came = lax.rem(jnp.where(part == 0, group[0], group[1]) + RING - step, RING)
    slot = jnp.minimum(part * 3 * RING + came * 3 + member, per - 1)
    found = waves_of((inner // RING) * per + slot)
    orders[...] = jnp.broadcast_to(found, orders.shape)

    lane = lax.broadcasted_iota(jnp.int32, (1, 128), 1).astype(jnp.float32)

    def make_basis(block):
        u = orders[pl.ds(pl.multiple_of(block * 64, 64), 64), :]
        half = jnp.floor(u * 0.5) * 2.0
        even = jnp.where(half == u, u, (HALF - 1.0) - u)
        for par in range(2):
            order = even if par == 0 else (HALF - 1.0) - even
            weight = jnp.where(order == 0.0, 1.0, 2.0)
            cos, sin = turn(order * lane)
            cos, sin = weight * cos, weight * sin
            cos_t, sin_t = turn(order * (lane * 128.0))
            for t in range(6):
                ct, st = cos_t[:, t : t + 1], sin_t[:, t : t + 1]
                for e, value in enumerate((cos * ct - sin * st, -(sin * ct + cos * st))):
                    hi, lo = split_bf16(value)
                    for j, item in enumerate((hi, hi, lo)):
                        basis[par, block, pl.ds(j * 128 + e * 64, 64), pl.ds(t * 128, 128)] = item

    def make_bases(start, count):
        lax.fori_loop(start, start + count, lambda n, c: (make_basis(n), c)[1], 0)

    column = lax.broadcasted_iota(jnp.int32, (1, table.shape[3]), 1)
    deg_dev = packs.shape[2] // 4
    deg = RING * deg_dev
    turned_column = (
        lax.rem(column, deg) // deg_dev * deg + column // deg * deg_dev + lax.rem(column, deg_dev)
    )
    natural = lax.broadcasted_iota(jnp.int32, perm.shape, 0)
    perm[...] = jnp.where(natural == turned_column, 1.0, 0.0).astype(jnp.bfloat16)
    made = 0
    make_bases(made, BASIS_STEPS[0])
    made += BASIS_STEPS[0]

    def ring_send(a, dirn, step, s):
        org = lax.rem(place[a] + (RING - step if dirn == 0 else step), RING)
        ref = coef_all.at[a, org, pl.ds(s * (deg // 2), deg // 2)]
        return remote(ref, ref, r_send.at[a], r_recv.at[a, dirn, step, s], next_to[a][dirn])

    def hops(dirn, s):
        return 4 if s == dirn else 3

    live = {}
    for a in range(2):
        own_c[a].wait()
        wait_bytes(packs_in.at[a, pl.ds(0, 7)], c_recv.at[a])
        wide[a] = packs_in[a].astype(jnp.float32)
        for s in range(RING):
            for t in range(4):
                piece = wide[a, s, pl.ds(t * deg_dev, deg_dev), :]
                coef_rows[a, pl.ds(s * deg_dev, deg_dev), pl.ds(t * 128, 128)] = piece
        coef_all[a, place[a]] = coef_rows[a].astype(jnp.bfloat16)
        for s in range(2):
            for dirn in range(2):
                live[a, dirn, 0, s] = ring_send(a, dirn, 0, s)

    def ring_step(a, step):
        for s in range(2):
            for dirn in range(2):
                if step <= hops(dirn, s):
                    live[a, dirn, step - 1, s].wait_recv()
                    if step < hops(dirn, s):
                        live[a, dirn, step, s] = ring_send(a, dirn, step, s)

    for step in range(1, 4):
        send_table(TABLE_STEPS[step])
        if BASIS_STEPS[step]:
            make_bases(made, BASIS_STEPS[step])
            made += BASIS_STEPS[step]
        for a in range(2):
            ring_step(a, step)

    row = lax.broadcasted_iota(jnp.int32, (32, 1), 0)
    member = jnp.minimum(jnp.where(row < 24, row // 8, (row - 24) // 2), 2)
    lane_in = lax.rem(lax.broadcasted_iota(jnp.int32, (1, 1, 512), 2), 256)
    lane_out = lax.broadcasted_iota(jnp.int32, (1, 256), 1)
    lane_left = lax.broadcasted_iota(jnp.int32, (1, 128), 1)

    def make_coded(a):
        ring_step(a, 4)
        own_l[a].wait()
        wait_bytes(table_in.at[a, pl.ds(0, 7)], l_recv.at[a])
        u = waves_of(ma * per + jnp.minimum(a * 3 * RING + group[a] * 3 + member, per - 1))
        cut = HALF - u
        even = jnp.floor(u * 0.5) * 2.0 == u
        bounds = (
            (jnp.where(even, 0.0, cut), jnp.where(even, cut, HALF + 1.0)),
            (jnp.where(even, cut, 0.0), jnp.where(even, HALF + 1.0, cut)),
        )
        if a == 0:
            rows_a = table_in[0].astype(jnp.float32)
            at = column
        else:
            flat = table_in[1].reshape(RING * 32, -1)
            rows_a = jnp.dot(flat, perm[...], preferred_element_type=jnp.float32).reshape(RING, 32, -1)
            at = turned_column
        at = at.astype(jnp.float32)
        rhs = coef_all[a].reshape(-1, 512)
        for par in range(2):
            low, high = bounds[par]
            keep = ((at >= low) & (at < high))[None]
            lhs = jnp.where(keep, rows_a, 0.0).astype(jnp.bfloat16).reshape(RING * 32, -1)
            sums = jnp.dot(lhs, rhs, preferred_element_type=jnp.float32)
            sums = sums.reshape(RING, 4, 8, 512)
            tail = sums[:, 3]
            two, four = pltpu.roll(tail, 6, 1), pltpu.roll(tail, 4, 1)
            parts = (
                (0, 8, (sums[:, 0], sums[:, 1], sums[:, 2])),
                (8, 2, (tail, two, four)),
            )
            for start, count, (s0, s1, s2) in parts:
                value = jnp.where(lane_in < CH, s0, jnp.where(lane_in < 2 * CH, s1, s2))
                value = jnp.where(lane_in < 3 * CH, value, 0.0)
                top = jnp.max(jnp.abs(value), axis=2, keepdims=True)
                power = jnp.ceil(jnp.log2(jnp.maximum(top, 1e-30)) + 1e-3)
                code = jnp.round(value * (jnp.exp2(-power) * 32767.0)).astype(jnp.int32)
                word = (code[:, :, :256] << 16) | (code[:, :, 256:] & 0xFFFF)
                word = jnp.where(lane_in[:, :, :256] < 3 * CH, word, power.astype(jnp.int32))
                raw[par, :, start : start + count, :] = word[:, :count]
        for p in range(RING):
            i0, cut = (5 * p) // 4, 21 * (p % 4)
            left = None
            for par in range(2):
                one, two = raw[par, :, i0, :], raw[par, :, i0 + 1, :]
                main = one
                if cut:
                    near = pltpu.roll(one, 256 - cut, 1)
                    main = jnp.where(lax.rem(lane_out, CH) < CH - cut, near, pltpu.roll(two, CH - cut, 1))
                main = jnp.where(lane_out < 3 * CH, main, jnp.where(lane_out == 3 * CH, one, two))
                for half in range(2):
                    coded[a, :, p * 5 + par * 2 + half, 0, :] = main[:, half * 128 : half * 128 + 128]
                for b in range(3):
                    shift = 63 * par - 63 * b - cut
                    item = (pltpu.roll(two, shift % 256, 1) if shift else two)[:, :128]
                    left = item if left is None else jnp.where(lane_left < 63 * par + 21 * b, left, item)
            coded[a, :, p * 5 + 4, 0, :] = left

    own_b = []
    own_m = []

    def send_coded(a):
        own_b.append(keep_local(coded.at[a, group[a]], back.at[a, 0], own_sem.at[2, a]))
        for k in range(7):
            p = to[a][k]
            remote(coded.at[a, p], back.at[a, k + 1], b_send.at[a], b_recv.at[a, (k + 1) // 4], peer(a, p))

    def forward(a, batch):
        if batch == 0:
            own_b[a].wait()
            wait_bytes(back.at[a, pl.ds(1, 3)], b_recv.at[a, 0])
        else:
            wait_bytes(back.at[a, pl.ds(4, 4)], b_recv.at[a, 1])
        four = pl.ds(4 * batch, 4)
        for p in ma_to:
            remote(
                back.at[a, four, pl.ds(5 * p, 5)], words.at[a, ma, four],
                m_send.at[a], m_recv.at[a], (lat, p),
            )
        own_m.append(keep_local(back.at[a, four, pl.ds(5 * ma, 5)], words.at[a, ma, four], own_sem.at[3 + batch, a]))

    limit = CH - 21 * lax.rem(ma, 4)

    def plane(a, k):
        return words[a, :, :, k, 0, :].reshape(64, 128)

    def unit(power):
        return jnp.exp2(power.astype(jnp.float32)) * (1.0 / 32767.0)

    def turned_rows(word, scale):
        real = (word >> 16).astype(jnp.float32) * scale
        imag = ((word << 16) >> 16).astype(jnp.float32) * scale
        return jnp.concatenate([real, imag], axis=0).T

    def synthesize(a):
        wait_bytes(words.at[a, pl.ds(0, 7)], m_recv.at[a])
        scales = []
        for par in range(2):
            first, second = plane(a, par * 2), plane(a, par * 2 + 1)
            scale0 = unit(second[:, 3 * CH - 128 : 3 * CH - 127])
            scale1 = unit(second[:, 3 * CH - 127 : 3 * CH - 126])
            scales.append(scale1)
            for half, word in enumerate((first, second)):
                scale = jnp.where(lax.rem(lane_left + half * 128, CH) < limit, scale0, scale1)
                turned[par, pl.ds(half * 128, 128), :] = turned_rows(word, scale)
        turned[2, pl.ds(0, 128), :] = turned_rows(plane(a, 4), jnp.where(lane_left < 63, scales[0], scales[1]))
        for par in range(2):
            for b in range(3):
                blocks[par, b, pl.ds(0, CH), :] = turned[par, pl.ds(b * CH, CH), :]
                blocks[par, b, pl.ds(CH, 21), :] = turned[2, pl.ds(63 * par + 21 * b, 21), :]
                hi, lo = split_bf16(blocks[par, b])
                for j, item in enumerate((hi, lo, hi)):
                    rows[par, :, pl.ds((b * 3 + j) * 128, 128)] = item
            term = jnp.dot(
                rows[par], basis[par, 3 * a : 3 * a + 3].reshape(1152, -1), preferred_element_type=jnp.float32
            )
            if a == 0:
                total[par] = term
            else:
                total[par] += term

    blocks[...] = jnp.zeros(blocks.shape, jnp.float32)
    make_coded(0)
    send_coded(0)
    make_coded(1)
    send_coded(1)
    for a in range(2):
        for batch in range(2):
            forward(a, batch)
    for copy in own_m:
        copy.wait()
    synthesize(0)
    synthesize(1)

    edge = HALF - 640
    even, odd = total[0], total[1]
    plus = even + odd
    minus = pltpu.roll(even - odd, edge, 1)
    count = out.shape[0]
    out[:, :640] = plus[:count, :640]
    out[:, 640:768] = jnp.where(lane_left < edge, plus[:, 640:], minus[:, :128])[:count]
    out[:, 768:1408] = minus[:count, 128:]
    out[:, 1408:] = minus[:count, : LON - 1408]

    seven = pl.ds(0, 7)
    for a in range(2):
        wait_bytes(packs_in.at[a, seven], c_send.at[a])
        wait_bytes(table_in.at[a, seven], l_send.at[a])
        wait_bytes(coef_all.at[a, seven], r_send.at[a])
        wait_bytes(back.at[a, seven], b_send.at[a])
        wait_bytes(words.at[a, seven], m_send.at[a])


def synth_call(waves, tables, packs):
    vmem = pl.BlockSpec(memory_space=pltpu.VMEM)
    dma = pltpu.SemaphoreType.DMA
    deg = packs.shape[2] // 4 * RING
    lats, slots, deg_all = tables.shape
    table = (2, RING, 32, deg_all)
    f32, bf16, s32 = jnp.float32, jnp.bfloat16, jnp.int32
    return pl.pallas_call(
        synth_kernel,
        out_shape=jax.ShapeDtypeStruct((105, LON), f32),
        in_specs=[vmem, pl.BlockSpec(memory_space=pltpu.HBM), vmem],
        out_specs=vmem,
        scratch_shapes=[
            pltpu.VMEM(tables.shape, bf16),
            pltpu.VMEM((lats * 48, deg_all), bf16),
            pltpu.VMEM((2, RING * 32, lats * 48), bf16),
            pltpu.VMEM(table, bf16),
            pltpu.VMEM(table, bf16),
            pltpu.VMEM(packs.shape, bf16),
            pltpu.VMEM(packs.shape, f32),
            pltpu.VMEM((2, deg, 512), f32),
            pltpu.VMEM((2, RING, deg, 512), bf16),
            pltpu.VMEM((2, RING, 10, 256), s32),
            pltpu.VMEM((2, RING, 5 * RING, 1, 128), s32),
            pltpu.VMEM((2, RING, 5 * RING, 1, 128), s32),
            pltpu.VMEM((2, RING, RING, 5, 1, 128), s32),
            pltpu.VMEM((deg_all, deg_all), bf16),
            pltpu.VMEM((6 * 64, 128), f32),
            pltpu.VMEM((2, 6, 384, 768), bf16),
            pltpu.VMEM((3, 256, 128), f32),
            pltpu.VMEM((2, 3, 112, 128), f32),
            pltpu.VMEM((2, 112, 1152), bf16),
            pltpu.VMEM((2, 112, 768), f32),
            dma((2,)), dma((2,)), dma((2,)), dma((2,)),
            dma((2,)), dma((2, 2, 4, 2)),
            dma((2,)), dma((2, 2)), dma((2,)), dma((2,)), dma((6, 2)),
        ],
        compiler_params=pltpu.CompilerParams(
            collective_id=0, has_side_effects=True, vmem_limit_bytes=48 << 20
        ),
        name="synth",
    )(waves, tables, packs)


def body(pair_wave, legendre, coefs):
    return synth_call(
        pair_wave.reshape(1, -1), jnp.transpose(legendre, (1, 0, 2)), pack_coefs(coefs)
    )


def solution(mesh):
    in_specs = (P(), P("ma", "lat", None), P("ma", "lat", None))
    out_specs = P(("lat", "ma"), None)
    return jax.shard_map(body, mesh=mesh, in_specs=in_specs, out_specs=out_specs, check_vma=False)
```

```python
import math

import jax
import jax.numpy as jnp
from jax import lax
from jax.experimental import pallas as pl
from jax.experimental.pallas import tpu as pltpu
from jax.sharding import PartitionSpec as P

LON = 1440
HALF = 720
RING = 8
ORDER = (1, 7, 2, 6, 3, 5, 4)
TABLE_STEPS = ((4, 5), (2, 3), (6,), (0, 1))
BASIS_STEPS = (3, 2, 1, 0)
CH = 84
SINE = [(-1.0) ** n / math.factorial(2 * n + 1) for n in range(6)]
COSINE = [(-1.0) ** n / math.factorial(2 * n) for n in range(7)]
MESH = pl.DeviceIdType.MESH


def poly(coefficients, square):
    value = jnp.float32(coefficients[-1])
    for coefficient in coefficients[-2::-1]:
        value = value * square + coefficient
    return value


def turn(phase):
    turns = jnp.round(phase * (1.0 / LON))
    angle = (phase - turns * LON) * (math.pi / LON)
    square = angle * angle
    sine = angle * poly(SINE, square)
    return 1.0 - 2.0 * (sine * sine), 2.0 * (sine * poly(COSINE, square))


def split_bf16(x):
    hi = x.astype(jnp.bfloat16)
    return hi, (x - hi.astype(jnp.float32)).astype(jnp.bfloat16)


def synth_kernel(
    waves_in, tables, coefs, out,
    waves, coef_raw, coef_flat, coef_pick, packs, table_raw, table_flat, pick, table, table_in, packs_in, wide, coef_rows, coef_all, raw, coded, back, words,
    perm, orders, basis, turned, blocks, rows, total,
    c_send, c_recv, l_send, l_recv, r_send, r_recv,
    b_send, b_recv, m_send, m_recv, own_sem,
):
    lat = lax.axis_index("lat")
    ma = lax.axis_index("ma")
    y = lat // RING
    z = lax.rem(lat, RING)
    group = (z, y)
    place = (y, z)
    to = [[lax.rem(group[a] + d, RING) for d in ORDER] for a in range(2)]
    ma_to = [lax.rem(ma + d, RING) for d in ORDER]

    def peer(a, p):
        return (y * RING + p, ma) if a == 0 else (p * RING + z, ma)

    next_to = [
        [peer(1 - a, lax.rem(place[a] + step, RING)) for step in (1, RING - 1)]
        for a in range(2)
    ]

    load_c = pltpu.make_async_copy(coefs, coef_raw, own_sem.at[5, 1])
    load_c.start()
    load = pltpu.make_async_copy(tables, table_raw, own_sem.at[5, 0])
    load.start()
    load_w = pltpu.make_async_copy(waves_in, waves, own_sem.at[6, 0])
    load_w.start()
    barrier = pltpu.get_barrier_semaphore()
    targets = [peer(a, p) for a in range(2) for p in to[a]] + [(lat, p) for p in ma_to]
    for target in targets:
        pl.semaphore_signal(barrier, inc=1, device_id=target, device_id_type=MESH)

    lats, slots, deg_all = tables.shape
    deg_dev, _, cols = coefs.shape
    stride = 48
    coef_flat[...] = jnp.zeros(coef_flat.shape, coef_flat.dtype)
    row = lax.broadcasted_iota(jnp.int32, (16 * 2 * RING, 1), 0)
    inner = lax.rem(row, 16)
    lanes = lax.broadcasted_iota(jnp.int32, (16 * 2 * RING, deg_dev * stride), 1)
    for b in range(3):
        want = jnp.where(inner < deg_dev, inner * stride + row // 16 * 3 + b, -1)
        coef_pick[b] = jnp.where(lanes == want, 1.0, 0.0).astype(jnp.bfloat16)
    load_c.wait()
    for i in range(deg_dev):
        coef_flat[pl.ds(i * stride, slots), :cols] = coef_raw[i]
    real, imag = None, None
    lane_c = lax.broadcasted_iota(jnp.int32, (1, 256), 1)
    for b in range(3):
        moved = jnp.dot(coef_pick[b], coef_flat[...], preferred_element_type=jnp.float32)
        first = pltpu.roll(moved, b * CH, 1) if b else moved
        second = pltpu.roll(moved, (b * CH - CH) % 256, 1) if b != 1 else moved
        here = (lane_c >= b * CH) & (lane_c < b * CH + CH)
        real = jnp.where(here, first, 0.0 if real is None else real)
        imag = jnp.where(here, second, 0.0 if imag is None else imag)
    for a in range(2):
        for g in range(RING):
            at = (a * RING + g) * 16
            for t in range(4):
                piece = (real if t < 2 else imag)[at : at + deg_dev, t % 2 * 128 : t % 2 * 128 + 128]
                wide[a, g, pl.ds(t * deg_dev, deg_dev), :] = piece
        packs[a] = wide[a].astype(jnp.bfloat16)
    pl.semaphore_wait(barrier, len(targets))

    def remote(src, dst, send, recv, target):
        copy = pltpu.make_async_remote_copy(
            src_ref=src, dst_ref=dst, send_sem=send, recv_sem=recv,
            device_id=target, device_id_type=MESH,
        )
        copy.start()
        return copy

    def keep_local(src, dst, sem):
        copy = pltpu.make_async_copy(src, dst, sem)
        copy.start()
        return copy

    def wait_bytes(ref, sem):
        pltpu.make_async_copy(ref, ref, sem).wait()

    for k in range(6, -1, -1):
        for a in range(2):
            p = to[a][k]
            remote(packs.at[a, p], packs_in.at[a, group[a]], c_send.at[a], c_recv.at[a], peer(a, p))
    own_c = [keep_local(packs.at[a, group[a]], packs_in.at[a, group[a]], own_sem.at[0, a]) for a in range(2)]

    table_flat[...] = jnp.zeros(table_flat.shape, table_flat.dtype)
    row = lax.broadcasted_iota(jnp.int32, (RING * 32, 1), 0)
    inner = lax.rem(row, 32)
    member = jnp.where(inner < 24, inner // 8, (inner - 24) // 2)
    at_lat = jnp.where(inner < 24, lax.rem(inner, 8), 8 + lax.rem(inner, 2))
    for a in range(2):
        want = at_lat * stride + a * 3 * RING + row // 32 * 3 + member
        want = jnp.where(inner < 30, want, -1)
        lanes = lax.broadcasted_iota(jnp.int32, (RING * 32, lats * stride), 1)
        pick[a] = jnp.where(lanes == want, 1.0, 0.0).astype(jnp.bfloat16)
    load.wait()
    for i in range(lats):
        table_flat[pl.ds(i * stride, slots), :] = table_raw[i]
    for a in range(2):
        moved = jnp.dot(pick[a], table_flat[...], preferred_element_type=jnp.float32)
        table[a] = moved.astype(jnp.bfloat16).reshape(RING, 32, deg_all)
    own_l = [keep_local(table.at[a, group[a]], table_in.at[a, group[a]], own_sem.at[1, a]) for a in range(2)]

    def send_table(ks):
        for k in ks:
            for a in range(2):
                p = to[a][k]
                remote(table.at[a, p], table_in.at[a, group[a]], l_send.at[a], l_recv.at[a], peer(a, p))

    send_table(TABLE_STEPS[0])

    pairs = waves.shape[0]
    per = pairs // RING
    load_w.wait()
    wave_row = waves[...].reshape(1, pairs).astype(jnp.float32)

    def waves_of(slot):
        lanes = lax.broadcasted_iota(jnp.int32, (slot.shape[0], pairs), 1)
        return jnp.sum(jnp.where(lanes == slot, wave_row, 0.0), axis=1, keepdims=True)

    row = lax.broadcasted_iota(jnp.int32, (6 * RING * RING, 1), 0)
    block, inner = row // (RING * RING), lax.rem(row, RING * RING)
    part, member = block // 3, lax.rem(block, 3)
    near = lax.rem(inner, RING)
    step = jnp.where(lax.rem(near, 2) == 1, (near + 1) // 2, RING - near // 2)
    came = lax.rem(jnp.where(part == 0, group[0], group[1]) + RING - step, RING)
    slot = jnp.minimum(part * 3 * RING + came * 3 + member, per - 1)
    found = waves_of((inner // RING) * per + slot)
    orders[...] = jnp.broadcast_to(found, orders.shape)

    lane = lax.broadcasted_iota(jnp.int32, (1, 128), 1).astype(jnp.float32)

    def make_basis(block):
        u = orders[pl.ds(pl.multiple_of(block * 64, 64), 64), :]
        half = jnp.floor(u * 0.5) * 2.0
        even = jnp.where(half == u, u, (HALF - 1.0) - u)
        for par in range(2):
            order = even if par == 0 else (HALF - 1.0) - even
            weight = jnp.where(order == 0.0, 1.0, 2.0)
            cos, sin = turn(order * lane)
            cos, sin = weight * cos, weight * sin
            cos_t, sin_t = turn(order * (lane * 128.0))
            for t in range(6):
                ct, st = cos_t[:, t : t + 1], sin_t[:, t : t + 1]
                for e, value in enumerate((cos * ct - sin * st, -(sin * ct + cos * st))):
                    hi, lo = split_bf16(value)
                    for j, item in enumerate((hi, hi, lo)):
                        basis[par, block, pl.ds(j * 128 + e * 64, 64), pl.ds(t * 128, 128)] = item

    def make_bases(start, count):
        lax.fori_loop(start, start + count, lambda n, c: (make_basis(n), c)[1], 0)

    column = lax.broadcasted_iota(jnp.int32, (1, table.shape[3]), 1)
    deg = RING * deg_dev
    turned_column = (
        lax.rem(column, deg) // deg_dev * deg + column // deg * deg_dev + lax.rem(column, deg_dev)
    )
    natural = lax.broadcasted_iota(jnp.int32, perm.shape, 0)
    perm[...] = jnp.where(natural == turned_column, 1.0, 0.0).astype(jnp.bfloat16)
    made = 0
    make_bases(made, BASIS_STEPS[0])
    made += BASIS_STEPS[0]

    def ring_send(a, dirn, step, s):
        org = lax.rem(place[a] + (RING - step if dirn == 0 else step), RING)
        ref = coef_all.at[a, org, pl.ds(s * (deg // 2), deg // 2)]
        return remote(ref, ref, r_send.at[a], r_recv.at[a, dirn, step, s], next_to[a][dirn])

    def hops(dirn, s):
        return 4 if s == dirn else 3

    live = {}
    for a in range(2):
        own_c[a].wait()
        wait_bytes(packs_in.at[a, pl.ds(0, 7)], c_recv.at[a])
        wide[a] = packs_in[a].astype(jnp.float32)
        for s in range(RING):
            for t in range(4):
                piece = wide[a, s, pl.ds(t * deg_dev, deg_dev), :]
                coef_rows[a, pl.ds(s * deg_dev, deg_dev), pl.ds(t * 128, 128)] = piece
        coef_all[a, place[a]] = coef_rows[a].astype(jnp.bfloat16)
        for s in range(2):
            for dirn in range(2):
                live[a, dirn, 0, s] = ring_send(a, dirn, 0, s)

    def ring_step(a, step):
        for s in range(2):
            for dirn in range(2):
                if step <= hops(dirn, s):
                    live[a, dirn, step - 1, s].wait_recv()
                    if step < hops(dirn, s):
                        live[a, dirn, step, s] = ring_send(a, dirn, step, s)

    for step in range(1, 4):
        send_table(TABLE_STEPS[step])
        if BASIS_STEPS[step]:
            make_bases(made, BASIS_STEPS[step])
            made += BASIS_STEPS[step]
        for a in range(2):
            ring_step(a, step)

    row = lax.broadcasted_iota(jnp.int32, (32, 1), 0)
    member = jnp.minimum(jnp.where(row < 24, row // 8, (row - 24) // 2), 2)
    lane_in = lax.rem(lax.broadcasted_iota(jnp.int32, (1, 1, 512), 2), 256)
    lane_out = lax.broadcasted_iota(jnp.int32, (1, 256), 1)
    lane_left = lax.broadcasted_iota(jnp.int32, (1, 128), 1)

    def make_coded(a):
        ring_step(a, 4)
        own_l[a].wait()
        wait_bytes(table_in.at[a, pl.ds(0, 7)], l_recv.at[a])
        u = waves_of(ma * per + jnp.minimum(a * 3 * RING + group[a] * 3 + member, per - 1))
        cut = HALF - u
        even = jnp.floor(u * 0.5) * 2.0 == u
        bounds = (
            (jnp.where(even, 0.0, cut), jnp.where(even, cut, HALF + 1.0)),
            (jnp.where(even, cut, 0.0), jnp.where(even, HALF + 1.0, cut)),
        )
        if a == 0:
            rows_a = table_in[0].astype(jnp.float32)
            at = column
        else:
            flat = table_in[1].reshape(RING * 32, -1)
            rows_a = jnp.dot(flat, perm[...], preferred_element_type=jnp.float32).reshape(RING, 32, -1)
            at = turned_column
        at = at.astype(jnp.float32)
        rhs = coef_all[a].reshape(-1, 512)
        for par in range(2):
            low, high = bounds[par]
            keep = ((at >= low) & (at < high))[None]
            lhs = jnp.where(keep, rows_a, 0.0).astype(jnp.bfloat16).reshape(RING * 32, -1)
            sums = jnp.dot(lhs, rhs, preferred_element_type=jnp.float32)
            sums = sums.reshape(RING, 4, 8, 512)
            tail = sums[:, 3]
            two, four = pltpu.roll(tail, 6, 1), pltpu.roll(tail, 4, 1)
            parts = (
                (0, 8, (sums[:, 0], sums[:, 1], sums[:, 2])),
                (8, 2, (tail, two, four)),
            )
            for start, count, (s0, s1, s2) in parts:
                value = jnp.where(lane_in < CH, s0, jnp.where(lane_in < 2 * CH, s1, s2))
                value = jnp.where(lane_in < 3 * CH, value, 0.0)
                top = jnp.max(jnp.abs(value), axis=2, keepdims=True)
                power = jnp.ceil(jnp.log2(jnp.maximum(top, 1e-30)) + 1e-3)
                code = jnp.round(value * (jnp.exp2(-power) * 32767.0)).astype(jnp.int32)
                word = (code[:, :, :256] << 16) | (code[:, :, 256:] & 0xFFFF)
                word = jnp.where(lane_in[:, :, :256] < 3 * CH, word, power.astype(jnp.int32))
                raw[par, :, start : start + count, :] = word[:, :count]
        for p in range(RING):
            i0, cut = (5 * p) // 4, 21 * (p % 4)
            left = None
            for par in range(2):
                one, two = raw[par, :, i0, :], raw[par, :, i0 + 1, :]
                main = one
                if cut:
                    near = pltpu.roll(one, 256 - cut, 1)
                    main = jnp.where(lax.rem(lane_out, CH) < CH - cut, near, pltpu.roll(two, CH - cut, 1))
                main = jnp.where(lane_out < 3 * CH, main, jnp.where(lane_out == 3 * CH, one, two))
                for half in range(2):
                    coded[a, :, p * 5 + par * 2 + half, 0, :] = main[:, half * 128 : half * 128 + 128]
                for b in range(3):
                    shift = 63 * par - 63 * b - cut
                    item = (pltpu.roll(two, shift % 256, 1) if shift else two)[:, :128]
                    left = item if left is None else jnp.where(lane_left < 63 * par + 21 * b, left, item)
            coded[a, :, p * 5 + 4, 0, :] = left

    own_b = []
    own_m = []

    def send_coded(a):
        own_b.append(keep_local(coded.at[a, group[a]], back.at[a, 0], own_sem.at[2, a]))
        for k in range(7):
            p = to[a][k]
            remote(coded.at[a, p], back.at[a, k + 1], b_send.at[a], b_recv.at[a, (k + 1) // 4], peer(a, p))

    def forward(a, batch):
        if batch == 0:
            own_b[a].wait()
            wait_bytes(back.at[a, pl.ds(1, 3)], b_recv.at[a, 0])
        else:
            wait_bytes(back.at[a, pl.ds(4, 4)], b_recv.at[a, 1])
        four = pl.ds(4 * batch, 4)
        for p in ma_to:
            remote(
                back.at[a, four, pl.ds(5 * p, 5)], words.at[a, ma, four],
                m_send.at[a], m_recv.at[a], (lat, p),
            )
        own_m.append(keep_local(back.at[a, four, pl.ds(5 * ma, 5)], words.at[a, ma, four], own_sem.at[3 + batch, a]))

    limit = CH - 21 * lax.rem(ma, 4)

    def plane(a, k):
        return words[a, :, :, k, 0, :].reshape(64, 128)

    def unit(power):
        return jnp.exp2(power.astype(jnp.float32)) * (1.0 / 32767.0)

    def turned_rows(word, scale):
        real = (word >> 16).astype(jnp.float32) * scale
        imag = ((word << 16) >> 16).astype(jnp.float32) * scale
        return jnp.concatenate([real, imag], axis=0).T

    def synthesize(a):
        wait_bytes(words.at[a, pl.ds(0, 7)], m_recv.at[a])
        scales = []
        for par in range(2):
            first, second = plane(a, par * 2), plane(a, par * 2 + 1)
            scale0 = unit(second[:, 3 * CH - 128 : 3 * CH - 127])
            scale1 = unit(second[:, 3 * CH - 127 : 3 * CH - 126])
            scales.append(scale1)
            for half, word in enumerate((first, second)):
                scale = jnp.where(lax.rem(lane_left + half * 128, CH) < limit, scale0, scale1)
                turned[par, pl.ds(half * 128, 128), :] = turned_rows(word, scale)
        turned[2, pl.ds(0, 128), :] = turned_rows(plane(a, 4), jnp.where(lane_left < 63, scales[0], scales[1]))
        for par in range(2):
            for b in range(3):
                blocks[par, b, pl.ds(0, CH), :] = turned[par, pl.ds(b * CH, CH), :]
                blocks[par, b, pl.ds(CH, 21), :] = turned[2, pl.ds(63 * par + 21 * b, 21), :]
                hi, lo = split_bf16(blocks[par, b])
                for j, item in enumerate((hi, lo, hi)):
                    rows[par, :, pl.ds((b * 3 + j) * 128, 128)] = item
            term = jnp.dot(
                rows[par], basis[par, 3 * a : 3 * a + 3].reshape(1152, -1), preferred_element_type=jnp.float32
            )
            if a == 0:
                total[par] = term
            else:
                total[par] += term

    blocks[...] = jnp.zeros(blocks.shape, jnp.float32)
    make_coded(0)
    send_coded(0)
    make_coded(1)
    send_coded(1)
    for a in range(2):
        for batch in range(2):
            forward(a, batch)
    for copy in own_m:
        copy.wait()
    synthesize(0)
    synthesize(1)

    edge = HALF - 640
    even, odd = total[0], total[1]
    plus = even + odd
    minus = pltpu.roll(even - odd, edge, 1)
    count = out.shape[0]
    out[:, :640] = plus[:count, :640]
    out[:, 640:768] = jnp.where(lane_left < edge, plus[:, 640:], minus[:, :128])[:count]
    out[:, 768:1408] = minus[:count, 128:]
    out[:, 1408:] = minus[:count, : LON - 1408]

    seven = pl.ds(0, 7)
    for a in range(2):
        wait_bytes(packs_in.at[a, seven], c_send.at[a])
        wait_bytes(table_in.at[a, seven], l_send.at[a])
        wait_bytes(coef_all.at[a, seven], r_send.at[a])
        wait_bytes(back.at[a, seven], b_send.at[a])
        wait_bytes(words.at[a, seven], m_send.at[a])


def synth_call(waves, tables, coefs):
    vmem = pl.BlockSpec(memory_space=pltpu.VMEM)
    dma = pltpu.SemaphoreType.DMA
    packs = (2, RING, 4 * coefs.shape[0], 128)
    deg = coefs.shape[0] * RING
    lats, slots, deg_all = tables.shape
    table = (2, RING, 32, deg_all)
    f32, bf16, s32 = jnp.float32, jnp.bfloat16, jnp.int32
    return pl.pallas_call(
        synth_kernel,
        out_shape=jax.ShapeDtypeStruct((105, LON), f32),
        in_specs=[pl.BlockSpec(memory_space=pltpu.HBM)] * 3,
        out_specs=vmem,
        scratch_shapes=[
            pltpu.VMEM(waves.shape, s32),
            pltpu.VMEM(coefs.shape, bf16),
            pltpu.VMEM((coefs.shape[0] * 48, 256), bf16),
            pltpu.VMEM((3, 16 * 2 * RING, coefs.shape[0] * 48), bf16),
            pltpu.VMEM(packs, bf16),
            pltpu.VMEM(tables.shape, bf16),
            pltpu.VMEM((lats * 48, deg_all), bf16),
            pltpu.VMEM((2, RING * 32, lats * 48), bf16),
            pltpu.VMEM(table, bf16),
            pltpu.VMEM(table, bf16),
            pltpu.VMEM(packs, bf16),
            pltpu.VMEM(packs, f32),
            pltpu.VMEM((2, deg, 512), f32),
            pltpu.VMEM((2, RING, deg, 512), bf16),
            pltpu.VMEM((2, RING, 10, 256), s32),
            pltpu.VMEM((2, RING, 5 * RING, 1, 128), s32),
            pltpu.VMEM((2, RING, 5 * RING, 1, 128), s32),
            pltpu.VMEM((2, RING, RING, 5, 1, 128), s32),
            pltpu.VMEM((deg_all, deg_all), bf16),
            pltpu.VMEM((6 * 64, 128), f32),
            pltpu.VMEM((2, 6, 384, 768), bf16),
            pltpu.VMEM((3, 256, 128), f32),
            pltpu.VMEM((2, 3, 112, 128), f32),
            pltpu.VMEM((2, 112, 1152), bf16),
            pltpu.VMEM((2, 112, 768), f32),
            dma((2,)), dma((2,)), dma((2,)), dma((2,)),
            dma((2,)), dma((2, 2, 4, 2)),
            dma((2,)), dma((2, 2)), dma((2,)), dma((2,)), dma((7, 2)),
        ],
        compiler_params=pltpu.CompilerParams(
            collective_id=0, has_side_effects=True, vmem_limit_bytes=48 << 20
        ),
        name="synth",
    )(waves, tables, coefs)


def body(pair_wave, legendre, coefs):
    tables, coefs = jnp.transpose(legendre, (1, 0, 2)), jnp.transpose(coefs, (1, 0, 2))
    args = (pair_wave, tables, coefs)
    return synth_call(*(pltpu.with_memory_space_constraint(x, pltpu.HBM) for x in args))


def solution(mesh):
    in_specs = (P(), P("ma", "lat", None), P("ma", "lat", None))
    out_specs = P(("lat", "ma"), None)
    return jax.shard_map(body, mesh=mesh, in_specs=in_specs, out_specs=out_specs, check_vma=False)
```

```python
import math

import jax
import jax.numpy as jnp
from jax import lax
from jax.experimental import pallas as pl
from jax.experimental.pallas import tpu as pltpu
from jax.sharding import PartitionSpec as P

LON = 1440
HALF = 720
RING = 8
ORDER = (1, 7, 2, 6, 3, 5, 4)
TABLE_STEPS = ((4, 5), (2, 3), (6,), (0, 1))
BASIS_STEPS = (3, 2, 1, 0)
CH = 84
SINE = [(-1.0) ** n / math.factorial(2 * n + 1) for n in range(6)]
COSINE = [(-1.0) ** n / math.factorial(2 * n) for n in range(7)]
MESH = pl.DeviceIdType.MESH


def poly(coefficients, square):
    value = jnp.float32(coefficients[-1])
    for coefficient in coefficients[-2::-1]:
        value = value * square + coefficient
    return value


def turn(phase):
    turns = jnp.round(phase * (1.0 / LON))
    angle = (phase - turns * LON) * (math.pi / LON)
    square = angle * angle
    sine = angle * poly(SINE, square)
    return 1.0 - 2.0 * (sine * sine), 2.0 * (sine * poly(COSINE, square))


def split_bf16(x):
    hi = x.astype(jnp.bfloat16)
    return hi, (x - hi.astype(jnp.float32)).astype(jnp.bfloat16)


def synth_kernel(
    waves_in, tables, coefs, out,
    waves, coef_raw, coef_flat, coef_pick, packs, table_raw, table_flat, pick, table, table_in, packs_in, wide, coef_rows, coef_all, raw, coded, back, words,
    masked, perm, orders, basis, turned, blocks, rows, total,
    c_send, c_recv, l_send, l_recv, r_send, r_recv,
    b_send, b_recv, m_send, m_recv, own_sem,
):
    lat = lax.axis_index("lat")
    ma = lax.axis_index("ma")
    y = lat // RING
    z = lax.rem(lat, RING)
    group = (z, y)
    place = (y, z)
    to = [[lax.rem(group[a] + d, RING) for d in ORDER] for a in range(2)]
    ma_to = [lax.rem(ma + d, RING) for d in ORDER]

    def peer(a, p):
        return (y * RING + p, ma) if a == 0 else (p * RING + z, ma)

    next_to = [
        [peer(1 - a, lax.rem(place[a] + step, RING)) for step in (1, RING - 1)]
        for a in range(2)
    ]

    load_c = pltpu.make_async_copy(coefs, coef_raw, own_sem.at[5, 1])
    load_c.start()
    load = pltpu.make_async_copy(tables, table_raw, own_sem.at[5, 0])
    load.start()
    load_w = pltpu.make_async_copy(waves_in, waves, own_sem.at[6, 0])
    load_w.start()
    barrier = pltpu.get_barrier_semaphore()
    targets = [peer(a, p) for a in range(2) for p in to[a]] + [(lat, p) for p in ma_to]
    for target in targets:
        pl.semaphore_signal(barrier, inc=1, device_id=target, device_id_type=MESH)

    lats, slots, deg_all = tables.shape
    deg_dev, _, cols = coefs.shape
    stride = 48
    coef_flat[...] = jnp.zeros(coef_flat.shape, coef_flat.dtype)
    row = lax.broadcasted_iota(jnp.int32, (16 * 2 * RING, 1), 0)
    inner = lax.rem(row, 16)
    lanes = lax.broadcasted_iota(jnp.int32, (16 * 2 * RING, deg_dev * stride), 1)
    for b in range(3):
        want = jnp.where(inner < deg_dev, inner * stride + row // 16 * 3 + b, -1)
        coef_pick[b] = jnp.where(lanes == want, 1.0, 0.0).astype(jnp.bfloat16)
    load_c.wait()
    for i in range(deg_dev):
        coef_flat[pl.ds(i * stride, slots), :cols] = coef_raw[i]
    real, imag = None, None
    lane_c = lax.broadcasted_iota(jnp.int32, (1, 256), 1)
    for b in range(3):
        moved = jnp.dot(coef_pick[b], coef_flat[...], preferred_element_type=jnp.float32)
        first = pltpu.roll(moved, b * CH, 1) if b else moved
        second = pltpu.roll(moved, (b * CH - CH) % 256, 1) if b != 1 else moved
        here = (lane_c >= b * CH) & (lane_c < b * CH + CH)
        real = jnp.where(here, first, 0.0 if real is None else real)
        imag = jnp.where(here, second, 0.0 if imag is None else imag)
    for a in range(2):
        for g in range(RING):
            at = (a * RING + g) * 16
            for t in range(4):
                piece = (real if t < 2 else imag)[at : at + deg_dev, t % 2 * 128 : t % 2 * 128 + 128]
                wide[a, g, pl.ds(t * deg_dev, deg_dev), :] = piece
        packs[a] = wide[a].astype(jnp.bfloat16)
    pl.semaphore_wait(barrier, len(targets))

    def remote(src, dst, send, recv, target):
        copy = pltpu.make_async_remote_copy(
            src_ref=src, dst_ref=dst, send_sem=send, recv_sem=recv,
            device_id=target, device_id_type=MESH,
        )
        copy.start()
        return copy

    def keep_local(src, dst, sem):
        copy = pltpu.make_async_copy(src, dst, sem)
        copy.start()
        return copy

    def wait_bytes(ref, sem):
        pltpu.make_async_copy(ref, ref, sem).wait()

    for k in range(6, -1, -1):
        for a in range(2):
            p = to[a][k]
            remote(packs.at[a, p], packs_in.at[a, group[a]], c_send.at[a], c_recv.at[a], peer(a, p))
    own_c = [keep_local(packs.at[a, group[a]], packs_in.at[a, group[a]], own_sem.at[0, a]) for a in range(2)]

    table_flat[...] = jnp.zeros(table_flat.shape, table_flat.dtype)
    row = lax.broadcasted_iota(jnp.int32, (RING * 32, 1), 0)
    inner = lax.rem(row, 32)
    member = jnp.where(inner < 24, inner // 8, (inner - 24) // 2)
    at_lat = jnp.where(inner < 24, lax.rem(inner, 8), 8 + lax.rem(inner, 2))
    for a in range(2):
        want = at_lat * stride + a * 3 * RING + row // 32 * 3 + member
        want = jnp.where(inner < 30, want, -1)
        lanes = lax.broadcasted_iota(jnp.int32, (RING * 32, lats * stride), 1)
        pick[a] = jnp.where(lanes == want, 1.0, 0.0).astype(jnp.bfloat16)
    load.wait()
    for i in range(lats):
        table_flat[pl.ds(i * stride, slots), :] = table_raw[i]
    for a in range(2):
        moved = jnp.dot(pick[a], table_flat[...], preferred_element_type=jnp.float32)
        table[a] = moved.astype(jnp.bfloat16).reshape(RING, 32, deg_all)
    own_l = [keep_local(table.at[a, group[a]], table_in.at[a, group[a]], own_sem.at[1, a]) for a in range(2)]

    def send_table(ks):
        for k in ks:
            for a in range(2):
                p = to[a][k]
                remote(table.at[a, p], table_in.at[a, group[a]], l_send.at[a], l_recv.at[a], peer(a, p))

    send_table(TABLE_STEPS[0])

    pairs = waves.shape[0]
    per = pairs // RING
    load_w.wait()
    wave_row = waves[...].reshape(1, pairs).astype(jnp.float32)

    def waves_of(slot):
        lanes = lax.broadcasted_iota(jnp.int32, (slot.shape[0], pairs), 1)
        return jnp.sum(jnp.where(lanes == slot, wave_row, 0.0), axis=1, keepdims=True)

    row = lax.broadcasted_iota(jnp.int32, (6 * RING * RING, 1), 0)
    block, inner = row // (RING * RING), lax.rem(row, RING * RING)
    part, member = block // 3, lax.rem(block, 3)
    near = lax.rem(inner, RING)
    step = jnp.where(lax.rem(near, 2) == 1, (near + 1) // 2, RING - near // 2)
    came = lax.rem(jnp.where(part == 0, group[0], group[1]) + RING - step, RING)
    slot = jnp.minimum(part * 3 * RING + came * 3 + member, per - 1)
    found = waves_of((inner // RING) * per + slot)
    orders[...] = jnp.broadcast_to(found, orders.shape)

    lane = lax.broadcasted_iota(jnp.int32, (1, 128), 1).astype(jnp.float32)

    def make_basis(block):
        u = orders[pl.ds(pl.multiple_of(block * 64, 64), 64), :]
        half = jnp.floor(u * 0.5) * 2.0
        even = jnp.where(half == u, u, (HALF - 1.0) - u)
        for par in range(2):
            order = even if par == 0 else (HALF - 1.0) - even
            weight = jnp.where(order == 0.0, 1.0, 2.0)
            cos, sin = turn(order * lane)
            cos, sin = weight * cos, weight * sin
            cos_t, sin_t = turn(order * (lane * 128.0))
            for t in range(6):
                ct, st = cos_t[:, t : t + 1], sin_t[:, t : t + 1]
                for e, value in enumerate((cos * ct - sin * st, -(sin * ct + cos * st))):
                    hi, lo = split_bf16(value)
                    for j, item in enumerate((hi, hi, lo)):
                        basis[par, block, pl.ds(j * 128 + e * 64, 64), pl.ds(t * 128, 128)] = item

    def make_bases(start, count):
        lax.fori_loop(start, start + count, lambda n, c: (make_basis(n), c)[1], 0)

    column = lax.broadcasted_iota(jnp.int32, (1, table.shape[3]), 1)
    deg = RING * deg_dev
    turned_column = (
        lax.rem(column, deg) // deg_dev * deg + column // deg * deg_dev + lax.rem(column, deg_dev)
    )
    natural = lax.broadcasted_iota(jnp.int32, perm.shape, 0)
    perm[...] = jnp.where(natural == turned_column, 1.0, 0.0).astype(jnp.bfloat16)
    made = 0
    make_bases(made, BASIS_STEPS[0])
    made += BASIS_STEPS[0]

    def ring_send(a, dirn, step, s):
        org = lax.rem(place[a] + (RING - step if dirn == 0 else step), RING)
        ref = coef_all.at[a, org, pl.ds(s * (deg // 2), deg // 2)]
        return remote(ref, ref, r_send.at[a], r_recv.at[a, dirn, step, s], next_to[a][dirn])

    def hops(dirn, s):
        return 4 if s == dirn else 3

    live = {}
    half_rows, half_ring = deg // 2, RING // 2
    for s in range(2):
        for a in range(2):
            if s == 0:
                own_c[a].wait()
                wait_bytes(packs_in.at[a, pl.ds(0, 7)], c_recv.at[a])
            part = pl.ds(s * half_ring, half_ring)
            wide[a, part] = packs_in[a, part].astype(jnp.float32)
            for n in range(s * half_ring, (s + 1) * half_ring):
                for t in range(4):
                    piece = wide[a, n, pl.ds(t * deg_dev, deg_dev), :]
                    coef_rows[a, pl.ds(n * deg_dev, deg_dev), pl.ds(t * 128, 128)] = piece
            part = pl.ds(s * half_rows, half_rows)
            coef_all[a, place[a], part] = coef_rows[a, part].astype(jnp.bfloat16)
            for dirn in range(2):
                live[a, dirn, 0, s] = ring_send(a, dirn, 0, s)

    def ring_step(a, step, s):
        for dirn in range(2):
            if step <= hops(dirn, s):
                live[a, dirn, step - 1, s].wait_recv()
                if step < hops(dirn, s):
                    live[a, dirn, step, s] = ring_send(a, dirn, step, s)

    for step in range(1, 4):
        send_table(TABLE_STEPS[step])
        if BASIS_STEPS[step]:
            make_bases(made, BASIS_STEPS[step])
            made += BASIS_STEPS[step]
        for s in range(2):
            for a in range(2):
                ring_step(a, step, s)

    row = lax.broadcasted_iota(jnp.int32, (32, 1), 0)
    member = jnp.minimum(jnp.where(row < 24, row // 8, (row - 24) // 2), 2)
    lane_in = lax.rem(lax.broadcasted_iota(jnp.int32, (1, 1, 512), 2), 256)
    lane_out = lax.broadcasted_iota(jnp.int32, (1, 256), 1)
    lane_left = lax.broadcasted_iota(jnp.int32, (1, 128), 1)

    def mask_table(a):
        own_l[a].wait()
        wait_bytes(table_in.at[a, pl.ds(0, 7)], l_recv.at[a])
        u = waves_of(ma * per + jnp.minimum(a * 3 * RING + group[a] * 3 + member, per - 1))
        cut = HALF - u
        even = jnp.floor(u * 0.5) * 2.0 == u
        bounds = (
            (jnp.where(even, 0.0, cut), jnp.where(even, cut, HALF + 1.0)),
            (jnp.where(even, cut, 0.0), jnp.where(even, HALF + 1.0, cut)),
        )
        if a == 0:
            rows_a = table_in[0].astype(jnp.float32)
            at = column
        else:
            flat = table_in[1].reshape(RING * 32, -1)
            rows_a = jnp.dot(flat, perm[...], preferred_element_type=jnp.float32).reshape(RING, 32, -1)
            at = turned_column
        at = at.astype(jnp.float32)
        for par in range(2):
            low, high = bounds[par]
            keep = ((at >= low) & (at < high))[None]
            masked[a, par] = jnp.where(keep, rows_a, 0.0).astype(jnp.bfloat16).reshape(RING * 32, -1)

    def make_coded(a):
        ring_step(a, 4, 0)
        ring_step(a, 4, 1)
        rhs = coef_all[a].reshape(-1, 512)
        for par in range(2):
            sums = jnp.dot(masked[a, par], rhs, preferred_element_type=jnp.float32)
            sums = sums.reshape(RING, 4, 8, 512)
            tail = sums[:, 3]
            two, four = pltpu.roll(tail, 6, 1), pltpu.roll(tail, 4, 1)
            parts = (
                (0, 8, (sums[:, 0], sums[:, 1], sums[:, 2])),
                (8, 2, (tail, two, four)),
            )
            for start, count, (s0, s1, s2) in parts:
                value = jnp.where(lane_in < CH, s0, jnp.where(lane_in < 2 * CH, s1, s2))
                value = jnp.where(lane_in < 3 * CH, value, 0.0)
                top = jnp.max(jnp.abs(value), axis=2, keepdims=True)
                power = jnp.ceil(jnp.log2(jnp.maximum(top, 1e-30)) + 1e-3)
                code = jnp.round(value * (jnp.exp2(-power) * 32767.0)).astype(jnp.int32)
                word = (code[:, :, :256] << 16) | (code[:, :, 256:] & 0xFFFF)
                word = jnp.where(lane_in[:, :, :256] < 3 * CH, word, power.astype(jnp.int32))
                raw[par, :, start : start + count, :] = word[:, :count]
        for p in range(RING):
            i0, cut = (5 * p) // 4, 21 * (p % 4)
            left = None
            for par in range(2):
                one, two = raw[par, :, i0, :], raw[par, :, i0 + 1, :]
                main = one
                if cut:
                    near = pltpu.roll(one, 256 - cut, 1)
                    main = jnp.where(lax.rem(lane_out, CH) < CH - cut, near, pltpu.roll(two, CH - cut, 1))
                main = jnp.where(lane_out < 3 * CH, main, jnp.where(lane_out == 3 * CH, one, two))
                for half in range(2):
                    coded[a, :, p * 5 + par * 2 + half, 0, :] = main[:, half * 128 : half * 128 + 128]
                for b in range(3):
                    shift = 63 * par - 63 * b - cut
                    item = (pltpu.roll(two, shift % 256, 1) if shift else two)[:, :128]
                    left = item if left is None else jnp.where(lane_left < 63 * par + 21 * b, left, item)
            coded[a, :, p * 5 + 4, 0, :] = left

    own_b = []
    own_m = []

    def send_coded(a):
        own_b.append(keep_local(coded.at[a, group[a]], back.at[a, 0], own_sem.at[2, a]))
        for k in range(7):
            p = to[a][k]
            remote(coded.at[a, p], back.at[a, k + 1], b_send.at[a], b_recv.at[a, (k + 1) // 4], peer(a, p))

    def forward(a, batch):
        if batch == 0:
            own_b[a].wait()
            wait_bytes(back.at[a, pl.ds(1, 3)], b_recv.at[a, 0])
        else:
            wait_bytes(back.at[a, pl.ds(4, 4)], b_recv.at[a, 1])
        four = pl.ds(4 * batch, 4)
        for p in ma_to:
            remote(
                back.at[a, four, pl.ds(5 * p, 5)], words.at[a, ma, four],
                m_send.at[a], m_recv.at[a], (lat, p),
            )
        own_m.append(keep_local(back.at[a, four, pl.ds(5 * ma, 5)], words.at[a, ma, four], own_sem.at[3 + batch, a]))

    limit = CH - 21 * lax.rem(ma, 4)

    def plane(a, k):
        return words[a, :, :, k, 0, :].reshape(64, 128)

    def unit(power):
        return jnp.exp2(power.astype(jnp.float32)) * (1.0 / 32767.0)

    def turned_rows(word, scale):
        real = (word >> 16).astype(jnp.float32) * scale
        imag = ((word << 16) >> 16).astype(jnp.float32) * scale
        return jnp.concatenate([real, imag], axis=0).T

    def synthesize(a):
        wait_bytes(words.at[a, pl.ds(0, 7)], m_recv.at[a])
        scales = []
        for par in range(2):
            first, second = plane(a, par * 2), plane(a, par * 2 + 1)
            scale0 = unit(second[:, 3 * CH - 128 : 3 * CH - 127])
            scale1 = unit(second[:, 3 * CH - 127 : 3 * CH - 126])
            scales.append(scale1)
            for half, word in enumerate((first, second)):
                scale = jnp.where(lax.rem(lane_left + half * 128, CH) < limit, scale0, scale1)
                turned[par, pl.ds(half * 128, 128), :] = turned_rows(word, scale)
        turned[2, pl.ds(0, 128), :] = turned_rows(plane(a, 4), jnp.where(lane_left < 63, scales[0], scales[1]))
        for par in range(2):
            for b in range(3):
                blocks[par, b, pl.ds(0, CH), :] = turned[par, pl.ds(b * CH, CH), :]
                blocks[par, b, pl.ds(CH, 21), :] = turned[2, pl.ds(63 * par + 21 * b, 21), :]
                hi, lo = split_bf16(blocks[par, b])
                for j, item in enumerate((hi, lo, hi)):
                    rows[par, :, pl.ds((b * 3 + j) * 128, 128)] = item
            term = jnp.dot(
                rows[par], basis[par, 3 * a : 3 * a + 3].reshape(1152, -1), preferred_element_type=jnp.float32
            )
            if a == 0:
                total[par] = term
            else:
                total[par] += term

    blocks[...] = jnp.zeros(blocks.shape, jnp.float32)
    mask_table(0)
    mask_table(1)
    make_coded(0)
    send_coded(0)
    make_coded(1)
    send_coded(1)
    for a in range(2):
        for batch in range(2):
            forward(a, batch)
    for copy in own_m:
        copy.wait()
    synthesize(0)
    synthesize(1)

    edge = HALF - 640
    even, odd = total[0], total[1]
    plus = even + odd
    minus = pltpu.roll(even - odd, edge, 1)
    count = out.shape[0]
    out[:, :640] = plus[:count, :640]
    out[:, 640:768] = jnp.where(lane_left < edge, plus[:, 640:], minus[:, :128])[:count]
    out[:, 768:1408] = minus[:count, 128:]
    out[:, 1408:] = minus[:count, : LON - 1408]

    seven = pl.ds(0, 7)
    for a in range(2):
        wait_bytes(packs_in.at[a, seven], c_send.at[a])
        wait_bytes(table_in.at[a, seven], l_send.at[a])
        wait_bytes(coef_all.at[a, seven], r_send.at[a])
        wait_bytes(back.at[a, seven], b_send.at[a])
        wait_bytes(words.at[a, seven], m_send.at[a])


def synth_call(waves, tables, coefs):
    vmem = pl.BlockSpec(memory_space=pltpu.VMEM)
    dma = pltpu.SemaphoreType.DMA
    packs = (2, RING, 4 * coefs.shape[0], 128)
    deg = coefs.shape[0] * RING
    lats, slots, deg_all = tables.shape
    table = (2, RING, 32, deg_all)
    f32, bf16, s32 = jnp.float32, jnp.bfloat16, jnp.int32
    return pl.pallas_call(
        synth_kernel,
        out_shape=jax.ShapeDtypeStruct((105, LON), f32),
        in_specs=[pl.BlockSpec(memory_space=pltpu.HBM)] * 3,
        out_specs=vmem,
        scratch_shapes=[
            pltpu.VMEM(waves.shape, s32),
            pltpu.VMEM(coefs.shape, bf16),
            pltpu.VMEM((coefs.shape[0] * 48, 256), bf16),
            pltpu.VMEM((3, 16 * 2 * RING, coefs.shape[0] * 48), bf16),
            pltpu.VMEM(packs, bf16),
            pltpu.VMEM(tables.shape, bf16),
            pltpu.VMEM((lats * 48, deg_all), bf16),
            pltpu.VMEM((2, RING * 32, lats * 48), bf16),
            pltpu.VMEM(table, bf16),
            pltpu.VMEM(table, bf16),
            pltpu.VMEM(packs, bf16),
            pltpu.VMEM(packs, f32),
            pltpu.VMEM((2, deg, 512), f32),
            pltpu.VMEM((2, RING, deg, 512), bf16),
            pltpu.VMEM((2, RING, 10, 256), s32),
            pltpu.VMEM((2, RING, 5 * RING, 1, 128), s32),
            pltpu.VMEM((2, RING, 5 * RING, 1, 128), s32),
            pltpu.VMEM((2, RING, RING, 5, 1, 128), s32),
            pltpu.VMEM((2, 2, RING * 32, deg_all), bf16),
            pltpu.VMEM((deg_all, deg_all), bf16),
            pltpu.VMEM((6 * 64, 128), f32),
            pltpu.VMEM((2, 6, 384, 768), bf16),
            pltpu.VMEM((3, 256, 128), f32),
            pltpu.VMEM((2, 3, 112, 128), f32),
            pltpu.VMEM((2, 112, 1152), bf16),
            pltpu.VMEM((2, 112, 768), f32),
            dma((2,)), dma((2,)), dma((2,)), dma((2,)),
            dma((2,)), dma((2, 2, 4, 2)),
            dma((2,)), dma((2, 2)), dma((2,)), dma((2,)), dma((7, 2)),
        ],
        compiler_params=pltpu.CompilerParams(
            collective_id=0, has_side_effects=True, vmem_limit_bytes=48 << 20
        ),
        name="synth",
    )(waves, tables, coefs)


def body(pair_wave, legendre, coefs):
    tables, coefs = jnp.transpose(legendre, (1, 0, 2)), jnp.transpose(coefs, (1, 0, 2))
    args = (pair_wave, tables, coefs)
    return synth_call(*(pltpu.with_memory_space_constraint(x, pltpu.HBM) for x in args))


def solution(mesh):
    in_specs = (P(), P("ma", "lat", None), P("ma", "lat", None))
    out_specs = P(("lat", "ma"), None)
    return jax.shard_map(body, mesh=mesh, in_specs=in_specs, out_specs=out_specs, check_vma=False)
```
